512 devices in a mesh: groups: 2 (over y), expert: 128 (over z, x), tensor: 2 (over core).
Axes of the slice: x: 8, y: 2, z: 16, core: 2. Of those that a mesh axis runs over, the one named last changes fastest.
The devices are a block of a 8x8x16 slice.
Arguments:
- tokens: bfloat16 [16384, 1536], P(('groups', 'expert')), parts along dimension 0, may hold values from -12 to 12
- gain: float32 [1536], replicated, may hold values from 0.25 to 1.75
- route_ids: int32 [16384, 4], P(('groups', 'expert')), parts along dimension 0, may hold values from 0 to 63, as said below
- route_weights: float32 [16384, 4], P(('groups', 'expert')), parts along dimension 0, may hold values from 0.05 to 0.5
- w_gate: bfloat16 [128, 1536, 768], P('expert', None, 'tensor'), may hold values from -0.15625 to 0.15625
- w_up: bfloat16 [128, 1536, 768], P('expert', None, 'tensor'), may hold values from -0.15625 to 0.15625
- w_down: bfloat16 [128, 768, 1536], P('expert', 'tensor'), may hold values from -0.15625 to 0.15625
Outputs:
- mixed: bfloat16 [16384, 1536], P(('groups', 'expert')), parts along dimension 0
The draws below stay inside these ranges and needn't reach their ends.
There are 2 independent parts, one for each index of `groups`. The reference program is written for one: setup_inputs(seed, part) draws one part's arguments, and reference() takes and returns one part's arrays. A program takes and returns all parts, laid end to end along the dimension named above; an argument that names none is the same for every part. Nothing has to cross between parts.
Inputs may be any that keep to these rules, and one draw needn't show every extreme that they name: `route_ids`: each row names 4 different experts. In each aligned block of 32 rows no expert is named more than 2 times; one expert, the same in every block, is named exactly 2 times in every block, and the other experts' counts within a block differ by at most one.
All inputs are finite; a program needn't handle non-finite values.
Results may differ from the reference program's by a relative error of at most 0.0045.
Values may be sent and summed in bfloat16 or wider, within the bound.
No kernel may reach another device: no remote copies, remote signals or barrier semaphores. Data moves between devices by JAX's collectives and lax.ppermute only.
A program may use at most 64 MiB of HBM per device.

```python
import math
import jax
import jax.numpy as jnp
from jax import lax

D = 1536
FF = 1536
TOP = 4
EXPERTS = 64
TOK_DEV = 32
CAP = 2
TOKENS = 8192


def draw_tokens(key, part):
    key_base = jax.random.fold_in(key, 0)
    values = jax.random.normal(key_base, (TOKENS, D), jnp.float32)
    return jnp.clip(values, -12.0, 12.0).astype(jnp.bfloat16)


def draw_route_ids(key, part):
    blocks = TOKENS // TOK_DEV
    slot_total = TOK_DEV * TOP
    others = EXPERTS - 1
    key_hot, key_rank, key_rows, key_cols = jax.random.split(key, 4)
    hot_expert = jax.random.randint(key_hot, (), 0, EXPERTS, dtype=jnp.int32)
    spare = slot_total - CAP
    floor_count = spare // others
    surplus = spare - floor_count * others
    rank_keys = jax.random.split(key_rank, blocks)
    ranking = jax.vmap(lambda sub_key: jax.random.permutation(sub_key, others))(rank_keys)
    counts = floor_count + (ranking < surplus).astype(jnp.int32)
    run_ends = CAP + jnp.cumsum(counts, axis=1, dtype=jnp.int32)
    places = jnp.arange(slot_total, dtype=jnp.int32)
    owner_index = jnp.sum((places[None, :, None] >= run_ends[:, None, :]).astype(jnp.int32), axis=2, dtype=jnp.int32)
    other_ids = (hot_expert + 1 + owner_index) % EXPERTS
    listed = jnp.where(places[None, :] < CAP, hot_expert, other_ids)
    id_grid = listed.reshape(blocks, TOP, TOK_DEV).transpose(0, 2, 1)
    row_keys = jax.random.split(key_rows, blocks)
    row_order = jax.vmap(lambda sub_key: jax.random.permutation(sub_key, TOK_DEV))(row_keys)
    id_grid = jnp.take_along_axis(id_grid, row_order[:, :, None], axis=1)
    scores = jax.random.randint(key_cols, (blocks, TOK_DEV, TOP), 0, 1 << 20, dtype=jnp.int32) * TOP + jnp.arange(TOP, dtype=jnp.int32)
    col_order = jnp.argsort(scores, axis=2)
    id_grid = jnp.take_along_axis(id_grid, col_order, axis=2)
    return id_grid.reshape(TOKENS, TOP).astype(jnp.int32)


def steps_of(own_key, dims, pieces, least, top_value):
    factor_of = 1.0
    for axis_at, parts in pieces:
        draws = jax.random.uniform(jax.random.fold_in(jax.random.fold_in(own_key, 6), axis_at), (parts,), jnp.float32, least / len(pieces), top_value / len(pieces))
        factor_of = factor_of * jnp.repeat(jnp.exp(draws), dims[axis_at] // parts).reshape((-1,) + (1,) * (len(dims) - 1 - axis_at))
    return factor_of


def normal_values(key, extent, deviation, limit, shards=(), held_as=jnp.bfloat16):
    level = steps_of(key, extent, shards, -0.22, 0.18) if shards else 1.0
    entries = jax.random.normal(key, extent, jnp.float32) * deviation * level
    return jnp.minimum(jnp.maximum(entries, -limit), limit).astype(held_as)


def setup_inputs(seed: int = 0, part: int = 0) -> dict:
    arg_keys = jax.random.split(jax.random.key(seed), 8)
    part_splits = jax.random.split(jax.random.fold_in(arg_keys[7], part), 8)
    tokens = draw_tokens(jax.random.fold_in(jax.random.fold_in(arg_keys[7], part), 71), part)
    gain = jnp.clip(1.0 + 0.15 * jax.random.normal(arg_keys[1], (D,), jnp.float32), 0.25, 1.75)
    route_ids = draw_route_ids(jax.random.fold_in(jax.random.fold_in(arg_keys[7], part), 71), part)
    route_weights = jnp.clip(jnp.exp(math.log(0.5) - 2.3025851 * jax.random.uniform(part_splits[3], (TOKENS, TOP), jnp.float32) ** steps_of(part_splits[3], (TOKENS, TOP), ((0, 128),), -0.2, 0.2)), 0.05, 0.5)
    w_gate = normal_values(arg_keys[4], (2 * EXPERTS, D, FF // 2), D ** -0.5, 0.15625, ((0, 128), (2, 2)))
    w_up = normal_values(arg_keys[5], (2 * EXPERTS, D, FF // 2), D ** -0.5, 0.15625, ((0, 128), (2, 2)))
    w_down = normal_values(arg_keys[6], (2 * EXPERTS, FF // 2, D), FF ** -0.5, 0.15625, ((0, 128), (1, 2)))
    return {"tokens": tokens, "gain": gain, "route_ids": route_ids, "route_weights": route_weights, "w_gate": w_gate, "w_up": w_up, "w_down": w_down}


def gated_unit(gate_val, up_val):
    return gate_val * jax.nn.sigmoid(1.702 * gate_val) * (up_val + 1.0)

def reference(tokens, gain, route_ids, route_weights, w_gate, w_up, w_down):
    resident = tokens.astype(jnp.float32)
    inv_rms = lax.rsqrt(lax.optimization_barrier(jnp.mean(resident * resident, axis=1, keepdims=True)) + 1e-05)
    normed = (resident * inv_rms * gain).astype(jnp.bfloat16)
    flat_ids = route_ids.reshape(-1)
    flat_weight = route_weights.reshape(-1)
    slot_total = flat_ids.shape[0]
    most_rows = TOKENS // TOK_DEV * CAP
    slot_range = jnp.arange(slot_total, dtype=jnp.int32)
    row_range = jnp.arange(most_rows, dtype=jnp.int32)

    def one_expert(summed, expert):
        chosen = flat_ids == expert
        rank_in = jnp.cumsum(chosen.astype(jnp.int32), dtype=jnp.int32) - 1
        target = jnp.where(chosen, rank_in, most_rows).astype(jnp.int32)
        picked = jnp.zeros((most_rows,), jnp.int32).at[target].set(slot_range, mode='drop')
        is_live = row_range < jnp.sum(chosen.astype(jnp.int32), dtype=jnp.int32)
        token_row = picked // TOP
        inputs = normed[token_row]
        first = (2 * expert).astype(jnp.int32)
        pair_gate = lax.dynamic_slice_in_dim(w_gate, first, 2, 0)
        pair_up = lax.dynamic_slice_in_dim(w_up, first, 2, 0)
        pair_down = lax.dynamic_slice_in_dim(w_down, first, 2, 0)
        full_gate = jnp.concatenate([pair_gate[0], pair_gate[1]], axis=1)
        full_up = jnp.concatenate([pair_up[0], pair_up[1]], axis=1)
        full_down = pair_down.reshape(-1, pair_down.shape[2])
        gate_val = jnp.dot(inputs, full_gate, preferred_element_type=jnp.float32)
        up_val = jnp.dot(inputs, full_up, preferred_element_type=jnp.float32)
        hidden = gated_unit(gate_val, up_val).astype(jnp.bfloat16)
        expert_out = jnp.dot(hidden, full_down, preferred_element_type=jnp.float32)
        weight = jnp.where(is_live, flat_weight[picked], 0.0)
        summed = summed.at[token_row].add(weight[:, None] * expert_out)
        return (summed, None)
    empty_sum = jnp.zeros(resident.shape, jnp.float32)
    summed, unused = lax.scan(one_expert, empty_sum, jnp.arange(EXPERTS, dtype=jnp.int32))
    return (resident + summed).astype(jnp.bfloat16)
```

```python
import jax
import jax.numpy as jnp
import numpy as np
from jax import lax
from jax.sharding import Mesh, PartitionSpec as P

X = 8


def gated_unit(gate_val, up_val):
    return gate_val * jax.nn.sigmoid(1.702 * gate_val) * (up_val + 1.0)


def route_tables(ids, weights, experts, room):
    rows, top = ids.shape
    matches = (ids[:, :, None] == jnp.arange(experts, dtype=jnp.int32)).astype(jnp.bfloat16)
    named = jnp.sum(matches, axis=1)
    earlier = (jnp.arange(rows)[:, None] > jnp.arange(rows)[None, :]).astype(jnp.bfloat16)
    before = jnp.dot(earlier, named, preferred_element_type=jnp.float32)
    position = jnp.sum(before[:, None, :] * matches.astype(jnp.float32), axis=2).astype(jnp.int32)
    slot = ids * room + position
    targets = jnp.arange(experts * room, dtype=jnp.int32)
    hits = slot[None, :, :] == targets[:, None, None]
    send = jnp.sum(hits.astype(jnp.float32), axis=2).astype(jnp.bfloat16)
    mix = jnp.sum(jnp.where(hits, weights[None, :, :], 0.0), axis=2)
    return send, mix


def per_device(tokens, gain, route_ids, route_weights, w_gate, w_up, w_down):
    zs = lax.axis_size("z")
    xs = lax.axis_size("x")
    cores = lax.axis_size("tensor")
    experts = zs * xs // 2
    pairs = xs // 2
    own = tokens.shape[0] // cores
    feats = tokens.shape[1]
    room = max(2, own * route_ids.shape[1] // experts)
    first = lax.axis_index("tensor") * own
    own_tokens = lax.dynamic_slice_in_dim(tokens, first, own, 0)
    own_ids = lax.dynamic_slice_in_dim(route_ids, first, own, 0)
    own_weights = lax.dynamic_slice_in_dim(route_weights, first, own, 0)
    resident = own_tokens.astype(jnp.float32)
    inv_rms = lax.rsqrt(jnp.mean(resident * resident, axis=1, keepdims=True) + 1e-05)
    normed = (resident * inv_rms * gain).astype(jnp.bfloat16)
    send, mix = route_tables(own_ids, own_weights, experts, room)
    slots = experts * room
    packed = jnp.dot(send, normed, preferred_element_type=jnp.float32).astype(jnp.bfloat16)
    arrived = lax.all_to_all(packed, "z", 0, 0, tiled=True)
    order = np.arange(slots).reshape(zs, pairs, room).transpose(1, 0, 2).reshape(pairs, 1, zs * room)
    order = np.broadcast_to(order, (pairs, 2, zs * room)).reshape(-1)
    spread = jnp.asarray(order[:, None] == np.arange(slots)[None, :], jnp.bfloat16)
    outgoing = jnp.dot(spread, arrived, preferred_element_type=jnp.float32).astype(jnp.bfloat16)
    rows = lax.all_to_all(outgoing, "x", 0, 0, tiled=True)
    swap = [(0, 1), (1, 0)]
    other = lax.ppermute(rows, "tensor", swap)
    both = jnp.concatenate([rows, other], axis=0)
    gate_val = jnp.dot(both, w_gate[0], preferred_element_type=jnp.float32)
    up_val = jnp.dot(both, w_up[0], preferred_element_type=jnp.float32)
    hidden = gated_unit(gate_val, up_val).astype(jnp.bfloat16)
    partial = jnp.dot(hidden, w_down[0], preferred_element_type=jnp.float32)
    n = rows.shape[0]
    theirs = lax.ppermute(partial[n:].astype(jnp.bfloat16), "tensor", swap)
    mine = (partial[:n] + theirs.astype(jnp.float32)).astype(jnp.bfloat16)
    back = lax.all_to_all(mine, "x", 0, 0, tiled=True)
    gathered = jnp.dot(spread.T, back, preferred_element_type=jnp.float32).astype(jnp.bfloat16)
    returned = lax.all_to_all(gathered, "z", 0, 0, tiled=True)
    weighted = jnp.dot(
        mix.T, returned.astype(jnp.float32), precision=lax.Precision.HIGHEST, preferred_element_type=jnp.float32
    )
    finished = (resident + weighted).astype(jnp.bfloat16)
    theirs_done = lax.ppermute(finished, "tensor", swap)
    low = lax.axis_index("tensor") == 0
    return jnp.concatenate(
        [jnp.where(low, finished, theirs_done), jnp.where(low, theirs_done, finished)], axis=0
    )


def solution(mesh):
    grid = Mesh(
        mesh.devices.reshape(mesh.devices.shape[0], -1, X, mesh.devices.shape[2]),
        ("groups", "z", "x", "tensor"),
    )
    rows = P(("groups", "z", "x"), None)
    placed = (
        rows,
        P(),
        rows,
        rows,
        P(("z", "x"), None, "tensor"),
        P(("z", "x"), None, "tensor"),
        P(("z", "x"), "tensor", None),
    )
    return jax.shard_map(
        per_device, mesh=grid, in_specs=placed, out_specs=rows, check_vma=False
    )
```

```python
import jax
import jax.numpy as jnp
import numpy as np
from jax import lax
from jax.sharding import Mesh, PartitionSpec as P

X = 8


def gated_unit(gate_val, up_val):
    return gate_val * jax.nn.sigmoid(1.702 * gate_val) * (up_val + 1.0)


def route_tables(ids, weights, experts, room):
    rows, top = ids.shape
    matches = (ids[:, :, None] == jnp.arange(experts, dtype=jnp.int32)).astype(jnp.bfloat16)
    named = jnp.sum(matches, axis=1)
    earlier = (jnp.arange(rows)[:, None] > jnp.arange(rows)[None, :]).astype(jnp.bfloat16)
    before = jnp.dot(earlier, named, preferred_element_type=jnp.float32)
    position = jnp.sum(before[:, None, :] * matches.astype(jnp.float32), axis=2).astype(jnp.int32)
    slot = ids * room + position
    targets = jnp.arange(experts * room, dtype=jnp.int32)
    hits = slot[None, :, :] == targets[:, None, None]
    send = jnp.sum(hits.astype(jnp.float32), axis=2).astype(jnp.bfloat16)
    mix = jnp.sum(jnp.where(hits, weights[None, :, :], 0.0), axis=2)
    return send, mix


def per_device(tokens, gain, route_ids, route_weights, w_gate, w_up, w_down):
    cores = lax.axis_size("tensor")
    experts = lax.axis_size("z") * lax.axis_size("pair")
    own = tokens.shape[0] // cores
    room = max(2, own * route_ids.shape[1] // experts)
    first = lax.axis_index("tensor") * own
    own_tokens = lax.dynamic_slice_in_dim(tokens, first, own, 0)
    own_ids = lax.dynamic_slice_in_dim(route_ids, first, own, 0)
    own_weights = lax.dynamic_slice_in_dim(route_weights, first, own, 0)
    resident = own_tokens.astype(jnp.float32)
    inv_rms = lax.rsqrt(jnp.mean(resident * resident, axis=1, keepdims=True) + 1e-05)
    normed = (resident * inv_rms * gain).astype(jnp.bfloat16)
    send, mix = route_tables(own_ids, own_weights, experts, room)
    packed = jnp.dot(send, normed, preferred_element_type=jnp.float32).astype(jnp.bfloat16)
    mine = lax.all_to_all(packed, ("z", "pair"), 0, 0, tiled=True)
    swap = [(0, 1), (1, 0)]
    theirs = lax.ppermute(mine, "half", swap)
    held, mine = lax.optimization_barrier(((w_gate[0], w_up[0], w_down[0]), mine))
    sent = tuple(lax.ppermute(w, "tensor", swap) for w in held)

    def through(rows):
        total = None
        for gate, up, down in (held, sent):
            gate_val = jnp.dot(rows, gate, preferred_element_type=jnp.float32)
            up_val = jnp.dot(rows, up, preferred_element_type=jnp.float32)
            hidden = gated_unit(gate_val, up_val).astype(jnp.bfloat16)
            part = jnp.dot(hidden, down, preferred_element_type=jnp.float32)
            total = part if total is None else total + part
        return total

    for_them = through(theirs).astype(jnp.bfloat16)
    from_them = lax.ppermute(for_them, "half", swap)
    summed = (through(mine) + from_them.astype(jnp.float32)).astype(jnp.bfloat16)
    returned = lax.all_to_all(summed, ("z", "pair"), 0, 0, tiled=True)
    weighted = jnp.dot(
        mix.T, returned.astype(jnp.float32), precision=lax.Precision.HIGHEST, preferred_element_type=jnp.float32
    )
    finished = (resident + weighted).astype(jnp.bfloat16)
    theirs_done = lax.ppermute(finished, "tensor", swap)
    low = lax.axis_index("tensor") == 0
    return jnp.concatenate(
        [jnp.where(low, finished, theirs_done), jnp.where(low, theirs_done, finished)], axis=0
    )


def solution(mesh):
    parts = mesh.devices.shape
    grid = Mesh(
        mesh.devices.reshape(parts[0], -1, X // 2, 2, parts[2]),
        ("groups", "z", "pair", "half", "tensor"),
    )
    chips = ("z", "pair", "half")
    rows = P(("groups", *chips), None)
    placed = (
        rows,
        P(),
        rows,
        rows,
        P(chips, None, "tensor"),
        P(chips, None, "tensor"),
        P(chips, "tensor", None),
    )
    return jax.shard_map(
        per_device, mesh=grid, in_specs=placed, out_specs=rows, check_vma=False
    )
```

```python
import jax
import jax.numpy as jnp
import numpy as np
from jax import lax
from jax.sharding import Mesh, PartitionSpec as P

X = 8


def gated_unit(gate_val, up_val):
    return gate_val * jax.nn.sigmoid(1.702 * gate_val) * (up_val + 1.0)


def slot_of(ids, experts, room):
    rows, top = ids.shape
    matches = (ids[:, :, None] == jnp.arange(experts, dtype=jnp.int32)).astype(jnp.bfloat16)
    named = jnp.sum(matches, axis=1)
    earlier = (jnp.arange(rows)[:, None] > jnp.arange(rows)[None, :]).astype(jnp.bfloat16)
    before = jnp.dot(earlier, named, preferred_element_type=jnp.float32)
    position = jnp.sum(before[:, None, :] * matches.astype(jnp.float32), axis=2).astype(jnp.int32)
    return ids * room + position


def per_device(tokens, gain, route_ids, route_weights, w_gate, w_up, w_down):
    zs = lax.axis_size("z")
    xs = lax.axis_size("x")
    cores = lax.axis_size("tensor")
    pairs = xs // 2
    experts = zs * pairs
    own = tokens.shape[0] // cores
    room = max(2, own * route_ids.shape[1] // experts)
    slots = experts * room
    first = lax.axis_index("tensor") * own
    own_tokens = lax.dynamic_slice_in_dim(tokens, first, own, 0)
    own_ids = lax.dynamic_slice_in_dim(route_ids, first, own, 0)
    own_weights = lax.dynamic_slice_in_dim(route_weights, first, own, 0)
    resident = own_tokens.astype(jnp.float32)
    inv_rms = lax.rsqrt(jnp.mean(resident * resident, axis=1, keepdims=True) + 1e-05)
    normed = (resident * inv_rms * gain).astype(jnp.bfloat16)
    slot = slot_of(own_ids, experts, room)
    targets = jnp.arange(slots, dtype=jnp.int32)
    send = jnp.sum((slot[None] == targets[:, None, None]).astype(jnp.float32), axis=2).astype(jnp.bfloat16)
    packed = jnp.dot(send, normed, preferred_element_type=jnp.float32).astype(jnp.bfloat16)
    arrived = lax.all_to_all(packed, "z", 0, 0, tiled=True)

    swap = [(0, 1), (1, 0)]
    held, own_slot, packed = lax.optimization_barrier(((w_gate[0], w_up[0], w_down[0]), slot, packed))
    sent = tuple(lax.ppermute(w, "tensor", swap) for w in held)
    place = lax.broadcasted_iota(jnp.int32, (xs * zs * room, slots), 0) + 0 * own_slot[0, 0]
    block, pos = place // (zs * room), place % (zs * room)
    source = (pos // room) * (pairs * room) + (block // 2) * room + pos % room
    spread = (source == lax.broadcasted_iota(jnp.int32, source.shape, 1)).astype(jnp.bfloat16)
    spread = lax.optimization_barrier(spread)
    outgoing = jnp.dot(spread, arrived, preferred_element_type=jnp.float32).astype(jnp.bfloat16)
    rows = lax.all_to_all(outgoing, "x", 0, 0, tiled=True)

    total = None
    for gate, up, down in (held, sent):
        gate_val = jnp.dot(rows, gate, preferred_element_type=jnp.float32)
        up_val = jnp.dot(rows, up, preferred_element_type=jnp.float32)
        hidden = gated_unit(gate_val, up_val).astype(jnp.bfloat16)
        part = jnp.dot(hidden, down, preferred_element_type=jnp.float32)
        total = part if total is None else total + part
    partial = total.astype(jnp.bfloat16)
    back = lax.all_to_all(partial, "x", 0, 0, tiled=True)
    late_slot, late_weights, _ = lax.optimization_barrier((slot, own_weights, partial))
    late_hits = late_slot[:, :, None] == targets[None, None, :]
    mix = jnp.sum(jnp.where(late_hits, late_weights[:, :, None], 0.0), axis=1)
    mix, back = lax.optimization_barrier((mix, back))
    gathered = jnp.dot(spread.T, back, preferred_element_type=jnp.float32).astype(jnp.bfloat16)
    returned = lax.all_to_all(gathered, "z", 0, 0, tiled=True)
    late_tokens, _ = lax.optimization_barrier((own_tokens, gathered))
    late_resident, returned = lax.optimization_barrier((late_tokens.astype(jnp.float32), returned))
    weighted = jnp.dot(
        mix, returned.astype(jnp.float32), precision=lax.Precision.HIGHEST, preferred_element_type=jnp.float32
    )
    finished = (late_resident + weighted).astype(jnp.bfloat16)
    theirs_done = lax.ppermute(finished, "tensor", swap)
    low = lax.axis_index("tensor") == 0
    return jnp.concatenate(
        [jnp.where(low, finished, theirs_done), jnp.where(low, theirs_done, finished)], axis=0
    )


def solution(mesh):
    grid = Mesh(
        mesh.devices.reshape(mesh.devices.shape[0], -1, X, mesh.devices.shape[2]),
        ("groups", "z", "x", "tensor"),
    )
    rows = P(("groups", "z", "x"), None)
    placed = (
        rows,
        P(),
        rows,
        rows,
        P(("z", "x"), None, "tensor"),
        P(("z", "x"), None, "tensor"),
        P(("z", "x"), "tensor", None),
    )
    return jax.shard_map(
        per_device, mesh=grid, in_specs=placed, out_specs=rows, check_vma=False
    )
```

```python
import functools

import jax
import jax.numpy as jnp
from jax import lax
from jax.experimental import pallas as pl
from jax.experimental.pallas import tpu as pltpu
from jax.sharding import Mesh, PartitionSpec as P

X = 8
CHUNKS = 2
VMEM = pl.BlockSpec(memory_space=pltpu.VMEM)
ANY = pl.BlockSpec(memory_space=pl.ANY)
F32 = jnp.float32
BF16 = jnp.bfloat16


def pack_kernel(own, room, tokens_ref, gain_ref, ids_ref, weights_ref, packed_ref, mix_ref):
    slots = packed_ref.shape[0]
    count = tokens_ref.shape[0]
    core = lax.axis_index("tensor")
    row = lax.broadcasted_iota(jnp.int32, (slots, count), 0)
    token = lax.broadcasted_iota(jnp.int32, (slots, count), 1)
    named = jnp.zeros((slots, count), F32)
    weight = jnp.zeros((slots, count), F32)
    for k in range(ids_ref.shape[0]):
        hit = ids_ref[k : k + 1, :] == row // room
        named = named + jnp.where(hit, 1.0, 0.0)
        weight = weight + jnp.where(hit, weights_ref[k : k + 1, :], 0.0)
    first = lax.broadcasted_iota(jnp.int32, (count, count), 0)
    second = lax.broadcasted_iota(jnp.int32, (count, count), 1)
    earlier = jnp.where((first < second) & (first // own == second // own), 1.0, 0.0)
    before = jnp.dot(named.astype(BF16), earlier.astype(BF16), preferred_element_type=F32)
    mask = (before == (row % room).astype(F32)) & (token // own == core)
    chosen = jnp.where(mask, named, 0.0)
    mix_ref[...] = jnp.where(mask, weight, 0.0)
    resident = tokens_ref[...].astype(F32)
    mean = jnp.mean(resident * resident, axis=1, keepdims=True)
    normed = (resident * lax.rsqrt(mean + 1e-05) * gain_ref[...][None, :]).astype(BF16)
    packed_ref[...] = jnp.dot(chosen.astype(BF16), normed, preferred_element_type=F32).astype(BF16)


def ffn_kernel(rows_ref, g0, u0, d0, g1, u1, d1, out_ref, gb, ub, db, sems):
    copies = []
    for i, (g, u, d) in enumerate(((g0, u0, d0), (g1, u1, d1))):
        for j, (src, dst) in enumerate(((g, gb.at[i]), (u, ub.at[i]), (d, db.at[i]))):
            copy = pltpu.make_async_copy(src, dst, sems.at[3 * i + j])
            copy.start()
            copies.append(copy)
    rows = rows_ref[...]
    total = None
    for i in range(2):
        copies[3 * i].wait()
        gate = jnp.dot(rows, gb[i], preferred_element_type=F32)
        copies[3 * i + 1].wait()
        up = jnp.dot(rows, ub[i], preferred_element_type=F32)
        hidden = (gate * jax.nn.sigmoid(1.702 * gate) * (up + 1.0)).astype(BF16)
        copies[3 * i + 2].wait()
        part = jnp.dot(hidden, db[i], preferred_element_type=F32)
        total = part if total is None else total + part
    out_ref[...] = total.astype(out_ref.dtype)


def finish_kernel(own, tokens_ref, mix_ref, returned_ref, out_ref):
    core = lax.axis_index("tensor")
    mix = mix_ref[...]
    rows = returned_ref[...]
    dims = (((0,), (0,)), ((), ()))
    high = mix.astype(BF16)
    rest = mix - high.astype(F32)
    mid = rest.astype(BF16)
    low = (rest - mid.astype(F32)).astype(BF16)
    weighted = sum(
        lax.dot_general(part, rows, dims, preferred_element_type=F32) for part in (low, mid, high)
    )
    done = (tokens_ref[...].astype(F32) + weighted).astype(BF16)
    out_ref[...] = jnp.where(core == 0, done[:own], done[own:])


def ffn(rows, weights, dtype):
    depth, width = weights[0].shape
    feats = rows.shape[1]
    flops = 2 * rows.shape[0] * 6 * depth * width
    return pl.pallas_call(
        ffn_kernel,
        out_shape=jax.ShapeDtypeStruct(rows.shape, dtype),
        in_specs=[VMEM] + [ANY] * 6,
        out_specs=VMEM,
        scratch_shapes=[
            pltpu.VMEM((2, depth, width), BF16),
            pltpu.VMEM((2, depth, width), BF16),
            pltpu.VMEM((2, width, feats), BF16),
            pltpu.SemaphoreType.DMA((6,)),
        ],
        compiler_params=pltpu.CompilerParams(vmem_limit_bytes=24 * 2**20),
        cost_estimate=pl.CostEstimate(flops=flops, bytes_accessed=12 * depth * width, transcendentals=0),
        name="ffn",
    )(rows, *weights)


def per_device(tokens, gain, route_ids, route_weights, w_gate, w_up, w_down):
    cores = lax.axis_size("tensor")
    experts = lax.axis_size("z") * lax.axis_size("pair")
    count, feats = tokens.shape
    own = count // cores
    room = max(2, own * route_ids.shape[1] // experts)
    slots = experts * room
    packed, mix = pl.pallas_call(
        functools.partial(pack_kernel, own, room),
        out_shape=(
            jax.ShapeDtypeStruct((slots, feats), BF16),
            jax.ShapeDtypeStruct((slots, count), F32),
        ),
        in_specs=[VMEM] * 4,
        out_specs=(VMEM, VMEM),
        compiler_params=pltpu.CompilerParams(vmem_limit_bytes=8 * 2**20),
        name="pack",
    )(tokens, gain, route_ids.T, route_weights.T)
    arrived = lax.all_to_all(packed, ("z", "pair"), 0, 0, tiled=True)
    swap = [(0, 1), (1, 0)]
    held, packed = lax.optimization_barrier(((w_gate[0], w_up[0], w_down[0]), packed))
    sent = tuple(lax.ppermute(w, "tensor", swap) for w in held)
    mine, sent = lax.optimization_barrier((arrived, sent))
    weights = (*held, *sent)
    step = slots // CHUNKS
    theirs = [
        lax.ppermute(mine[i * step : (i + 1) * step], "half", swap) for i in range(CHUNKS)
    ]
    from_them = []
    for rows in theirs:
        from_them.append(lax.ppermute(ffn(rows, weights, BF16), "half", swap))
    ours = ffn(mine, weights, F32)
    summed = (ours + jnp.concatenate(from_them, axis=0).astype(F32)).astype(BF16)
    returned = lax.all_to_all(summed, ("z", "pair"), 0, 0, tiled=True)
    finished = pl.pallas_call(
        functools.partial(finish_kernel, own),
        out_shape=jax.ShapeDtypeStruct((own, feats), BF16),
        in_specs=[VMEM] * 3,
        out_specs=VMEM,
        compiler_params=pltpu.CompilerParams(vmem_limit_bytes=8 * 2**20),
        name="finish",
    )(tokens, mix, returned)
    theirs_done = lax.ppermute(finished, "tensor", swap)
    low = lax.axis_index("tensor") == 0
    return jnp.concatenate(
        [jnp.where(low, finished, theirs_done), jnp.where(low, theirs_done, finished)], axis=0
    )


def solution(mesh):
    parts = mesh.devices.shape
    grid = Mesh(
        mesh.devices.reshape(parts[0], -1, X // 2, 2, parts[2]),
        ("groups", "z", "pair", "half", "tensor"),
    )
    chips = ("z", "pair", "half")
    rows = P(("groups", *chips), None)
    placed = (
        rows,
        P(),
        rows,
        rows,
        P(chips, None, "tensor"),
        P(chips, None, "tensor"),
        P(chips, "tensor", None),
    )
    return jax.shard_map(
        per_device, mesh=grid, in_specs=placed, out_specs=rows, check_vma=False
    )
```

```python
import functools

import jax
import jax.numpy as jnp
from jax import lax
from jax.experimental import pallas as pl
from jax.experimental.pallas import tpu as pltpu
from jax.sharding import Mesh, PartitionSpec as P

X = 8
CHUNKS = 2
CUTS = 4
VMEM = pl.BlockSpec(memory_space=pltpu.VMEM)
HBM = pl.BlockSpec(memory_space=pltpu.HBM)
F32 = jnp.float32
BF16 = jnp.bfloat16
ROWS_FIRST = (((0,), (0,)), ((), ()))


def routing(own, room, lines, ids, weights):
    count = ids.shape[1]
    core = lax.axis_index("tensor")
    line = lax.broadcasted_iota(jnp.int32, (lines, count), 0)
    token = lax.broadcasted_iota(jnp.int32, (lines, count), 1)
    expert = line // (room * CUTS)
    named = jnp.zeros((lines, count), F32)
    weight = jnp.zeros((lines, count), F32)
    for k in range(ids.shape[0]):
        hit = ids[k : k + 1, :] == expert
        named = named + jnp.where(hit, 1.0, 0.0)
        if weights is not None:
            weight = weight + jnp.where(hit, weights[k : k + 1, :], 0.0)
    first = lax.broadcasted_iota(jnp.int32, (count, count), 0)
    second = lax.broadcasted_iota(jnp.int32, (count, count), 1)
    earlier = jnp.where((first < second) & (first // own == second // own), 1.0, 0.0)
    before = jnp.dot(named.astype(BF16), earlier.astype(BF16), preferred_element_type=F32)
    here = (before == ((line // CUTS) % room).astype(F32)) & (token // own == core)
    return jnp.where(here, named, 0.0), jnp.where(here, weight, 0.0), line % CUTS


def pack_kernel(own, room, tokens_hbm, gain_hbm, ids_hbm, packed_ref, tokens_ref, gain_ref, ids_ref, sems):
    copies = [
        pltpu.make_async_copy(src, dst, sems.at[i])
        for i, (src, dst) in enumerate(
            ((ids_hbm, ids_ref), (tokens_hbm, tokens_ref), (gain_hbm, gain_ref))
        )
    ]
    for copy in copies:
        copy.start()
    copies[0].wait()
    lines, width = packed_ref.shape
    chosen, _, _ = routing(own, room, lines, ids_ref[...], None)
    chosen = chosen.astype(BF16)
    copies[1].wait()
    resident = tokens_ref[...].astype(F32)
    mean = jnp.mean(resident * resident, axis=1, keepdims=True)
    scaled = resident * lax.rsqrt(mean + 1e-05)
    copies[2].wait()
    normed = (scaled * gain_ref[...][None, :]).astype(BF16)
    cut = lax.broadcasted_iota(jnp.int32, (lines, width), 0) % CUTS
    packed = None
    for q in range(CUTS):
        part = jnp.dot(chosen, normed[:, q * width : (q + 1) * width], preferred_element_type=F32)
        packed = part if packed is None else jnp.where(cut == q, part, packed)
    packed_ref[...] = packed.astype(BF16)


def ffn_kernel(rows_ref, g0, u0, d0, g1, u1, d1, out_ref, gates, ups, downs, sems):
    copies = []
    for i, (g, u, d) in enumerate(((g0, u0, d0), (g1, u1, d1))):
        for src, dst in ((g, gates.at[i]), (u, ups.at[i]), (d, downs.at[i])):
            copies.append(pltpu.make_async_copy(src, dst, sems.at[len(copies)]))
    for i in (0, 1, 3, 4, 2, 5):
        copies[i].start()
    lines, width = rows_ref.shape
    count = lines // CUTS
    row = lax.broadcasted_iota(jnp.int32, (count, lines), 0)
    line = lax.broadcasted_iota(jnp.int32, (count, lines), 1)
    held = rows_ref[...]
    rows = jnp.concatenate(
        [
            jnp.dot(
                jnp.where(line == row * CUTS + q, 1.0, 0.0).astype(BF16), held, preferred_element_type=F32
            ).astype(BF16)
            for q in range(CUTS)
        ],
        axis=1,
    )
    hidden = []
    for i in range(2):
        copies[3 * i].wait()
        gate = jnp.dot(rows, gates[i], preferred_element_type=F32)
        copies[3 * i + 1].wait()
        up = jnp.dot(rows, ups[i], preferred_element_type=F32)
        hidden.append((gate * jax.nn.sigmoid(1.702 * gate) * (up + 1.0)).astype(BF16))
    total = None
    for i in range(2):
        copies[3 * i + 2].wait()
        part = jnp.dot(hidden[i], downs[i], preferred_element_type=F32)
        total = part if total is None else total + part
    out_ref[...] = total.astype(out_ref.dtype)


def join_kernel(ours_ref, *refs):
    *theirs, out_ref = refs
    lines, width = out_ref.shape
    count = lines // CUTS
    line = lax.broadcasted_iota(jnp.int32, (lines, count), 0)
    row = lax.broadcasted_iota(jnp.int32, (lines, count), 1)
    total = jnp.concatenate([r[...] for r in theirs], axis=0).astype(F32) + ours_ref[...]
    total = total.astype(BF16)
    out = None
    for q in range(CUTS):
        put = jnp.where(line == row * CUTS + q, 1.0, 0.0).astype(BF16)
        part = jnp.dot(put, total[:, q * width : (q + 1) * width], preferred_element_type=F32)
        out = part if out is None else out + part
    out_ref[...] = out.astype(BF16)


def finish_kernel(own, room, tokens_ref, ids_ref, weights_ref, returned_ref, out_ref):
    core = lax.axis_index("tensor")
    lines, width = returned_ref.shape
    _, mix, cut = routing(own, room, lines, ids_ref[...], weights_ref[...])
    rows = returned_ref[...]
    for q in range(CUTS):
        at = slice(q * width, (q + 1) * width)
        part = jnp.where(cut == q, mix, 0.0)
        high = part.astype(BF16)
        rest = part - high.astype(F32)
        mid = rest.astype(BF16)
        low = (rest - mid.astype(F32)).astype(BF16)
        weighted = sum(
            lax.dot_general(m, rows, ROWS_FIRST, preferred_element_type=F32) for m in (low, mid, high)
        )
        done = (tokens_ref[:, at].astype(F32) + weighted).astype(BF16)
        out_ref[:, at] = jnp.where(core == 0, done[:own], done[own:])


def small(limit):
    return pltpu.CompilerParams(vmem_limit_bytes=limit * 2**20)


def ffn(rows, weights, dtype):
    depth, width = weights[0].shape
    flops = 12 * (rows.shape[0] // CUTS) * depth * width
    return pl.pallas_call(
        ffn_kernel,
        out_shape=jax.ShapeDtypeStruct((rows.shape[0] // CUTS, depth), dtype),
        in_specs=[VMEM] + [HBM] * 6,
        out_specs=VMEM,
        scratch_shapes=[
            pltpu.VMEM((2, depth, width), BF16),
            pltpu.VMEM((2, depth, width), BF16),
            pltpu.VMEM((2, width, depth), BF16),
            pltpu.SemaphoreType.DMA((6,)),
        ],
        compiler_params=pltpu.CompilerParams(vmem_limit_bytes=53200 * 1024),
        cost_estimate=pl.CostEstimate(flops=flops, bytes_accessed=12 * depth * width, transcendentals=0),
        name="ffn",
    )(rows, *weights)


def per_device(tokens, gain, route_ids, route_weights, w_gate, w_up, w_down):
    cores = lax.axis_size("tensor")
    peers = lax.axis_size("z") * lax.axis_size("pair")
    count, feats = tokens.shape
    own = count // cores
    room = max(2, own * route_ids.shape[1] // peers)
    lines, width = peers * room * CUTS, feats // CUTS
    ids, mixing = route_ids.T, route_weights.T
    packed = pl.pallas_call(
        functools.partial(pack_kernel, own, room),
        out_shape=jax.ShapeDtypeStruct((lines, width), BF16),
        in_specs=[HBM] * 3,
        out_specs=VMEM,
        scratch_shapes=[
            pltpu.VMEM(tokens.shape, tokens.dtype),
            pltpu.VMEM(gain.shape, gain.dtype),
            pltpu.VMEM(ids.shape, ids.dtype),
            pltpu.SemaphoreType.DMA((3,)),
        ],
        name="pack",
    )(tokens, gain, ids)
    blocks = (peers, room * CUTS, width)
    mine = lax.all_to_all(packed.reshape(blocks), ("z", "pair"), 0, 0, tiled=True)
    swap = [(0, 1), (1, 0)]
    held, packed = lax.optimization_barrier(((w_gate[0], w_up[0], w_down[0]), packed))
    sent = tuple(lax.ppermute(w, "tensor", swap) for w in held)
    mine, sent = lax.optimization_barrier((mine, sent))
    mine = mine.reshape(lines, width)
    weights = (*held, *sent)
    step = lines // CHUNKS
    theirs = [
        lax.ppermute(mine[i * step : (i + 1) * step], "half", swap) for i in range(CHUNKS)
    ]
    from_them = [lax.ppermute(ffn(rows, weights, BF16), "half", swap) for rows in theirs]
    ours = ffn(mine, weights, F32)
    summed = pl.pallas_call(
        join_kernel,
        out_shape=jax.ShapeDtypeStruct((lines, width), BF16),
        in_specs=[VMEM] * (1 + CHUNKS),
        out_specs=VMEM,
        compiler_params=small(8),
        name="join",
    )(ours, *from_them)
    returned = lax.all_to_all(summed.reshape(blocks), ("z", "pair"), 0, 0, tiled=True)
    finished = pl.pallas_call(
        functools.partial(finish_kernel, own, room),
        out_shape=jax.ShapeDtypeStruct((own, feats), BF16),
        in_specs=[VMEM] * 4,
        out_specs=VMEM,
        compiler_params=small(8),
        name="finish",
    )(tokens, ids, mixing, returned.reshape(lines, width))
    theirs_done = lax.ppermute(finished, "tensor", swap)
    low = lax.axis_index("tensor") == 0
    return jnp.concatenate(
        [jnp.where(low, finished, theirs_done), jnp.where(low, theirs_done, finished)], axis=0
    )


def solution(mesh):
    parts = mesh.devices.shape
    grid = Mesh(
        mesh.devices.reshape(parts[0], -1, X // 2, 2, parts[2]),
        ("groups", "z", "pair", "half", "tensor"),
    )
    chips = ("z", "pair", "half")
    rows = P(("groups", *chips), None)
    placed = (
        rows,
        P(),
        rows,
        rows,
        P(chips, None, "tensor"),
        P(chips, None, "tensor"),
        P(chips, "tensor", None),
    )
    return jax.shard_map(
        per_device, mesh=grid, in_specs=placed, out_specs=rows, check_vma=False
    )
```

```python
import functools

import jax
import jax.numpy as jnp
from jax import lax
from jax.experimental import pallas as pl
from jax.experimental.pallas import tpu as pltpu
from jax.sharding import Mesh, PartitionSpec as P

X = 8
CHUNKS = 2
CUTS = 4
VMEM = pl.BlockSpec(memory_space=pltpu.VMEM)
HBM = pl.BlockSpec(memory_space=pltpu.HBM)
F32 = jnp.float32
BF16 = jnp.bfloat16
ROWS_FIRST = (((0,), (0,)), ((), ()))


def split(index, by):
    if by & (by - 1) == 0:
        return lax.shift_right_logical(index, by.bit_length() - 1), index & (by - 1)
    quotient = lax.div(index, by)
    return quotient, index - quotient * by


def routing(own, room, cuts, lines, ids, weights):
    count = ids.shape[1] // cuts
    core = lax.axis_index("tensor")
    line = lax.broadcasted_iota(jnp.int32, (lines, cuts * count), 0)
    column = lax.broadcasted_iota(jnp.int32, (lines, cuts * count), 1)
    slot, cut = split(line, cuts)
    expert, position = split(slot, room)
    of_cut, token = split(column, count)
    named = jnp.zeros(line.shape, F32)
    value = jnp.zeros(line.shape, F32)
    for k in range(ids.shape[0]):
        hit = ids[k : k + 1, :] == expert
        named = named + jnp.where(hit, 1.0, 0.0)
        if weights is not None:
            value = value + jnp.where(hit, weights[k : k + 1, :], 0.0)
    first = lax.broadcasted_iota(jnp.int32, (cuts * count,) * 2, 0)
    second = lax.broadcasted_iota(jnp.int32, (cuts * count,) * 2, 1)
    same_block = split(first, own)[0] == split(second, own)[0]
    earlier = jnp.where((first < second) & same_block, 1.0, 0.0).astype(BF16)
    before = jnp.dot(named.astype(BF16), earlier, preferred_element_type=F32)
    here = (before == position.astype(F32)) & (split(token, own)[0] == core) & (of_cut == cut)
    return jnp.where(here, named if weights is None else value, 0.0)


def pack_kernel(own, room, tokens_hbm, gain_hbm, ids_hbm, packed_ref, tokens_ref, gain_ref, ids_ref, sems):
    copies = [
        pltpu.make_async_copy(src, dst, sems.at[i])
        for i, (src, dst) in enumerate(
            ((ids_hbm, ids_ref), (tokens_hbm, tokens_ref), (gain_hbm, gain_ref))
        )
    ]
    for copy in copies:
        copy.start()
    copies[0].wait()
    lines, width = packed_ref.shape
    ids = jnp.concatenate([ids_ref[...]] * CUTS, axis=1)
    chosen = routing(own, room, CUTS, lines, ids, None).astype(BF16)
    copies[1].wait()
    resident = tokens_ref[...].astype(F32)
    mean = jnp.mean(resident * resident, axis=1, keepdims=True)
    scaled = resident * lax.rsqrt(mean + 1e-05)
    copies[2].wait()
    normed = (scaled * gain_ref[...][None, :]).astype(BF16)
    stacked = jnp.concatenate([normed[:, q * width : (q + 1) * width] for q in range(CUTS)], axis=0)
    packed_ref[...] = jnp.dot(chosen, stacked, preferred_element_type=F32).astype(BF16)


def mix_kernel(own, room, ids_ref, weights_ref, mix_ref):
    core = lax.axis_index("tensor")
    slots = mix_ref.shape[1]
    mix = routing(own, room, 1, slots, ids_ref[...], weights_ref[...]).T
    mix = jnp.where(core == 0, mix[:own], mix[own:])
    high = mix.astype(BF16)
    rest = mix - high.astype(F32)
    mid = rest.astype(BF16)
    mix_ref[...] = jnp.concatenate([high, mid, (rest - mid.astype(F32)).astype(BF16)], axis=0)


def uncut(held):
    lines, width = held.shape
    count = lines // CUTS
    row = lax.broadcasted_iota(jnp.int32, (count, lines), 0)
    line = lax.broadcasted_iota(jnp.int32, (count, lines), 1)
    return jnp.concatenate(
        [
            jnp.dot(
                jnp.where(line == row * CUTS + q, 1.0, 0.0).astype(BF16), held, preferred_element_type=F32
            ).astype(BF16)
            for q in range(CUTS)
        ],
        axis=1,
    )


def ffn_kernel(rows_ref, g0, u0, d0, g1, u1, d1, out_ref, gates, ups, downs, sems):
    copies = []
    for i, (g, u, d) in enumerate(((g0, u0, d0), (g1, u1, d1))):
        for src, dst in ((g, gates.at[i]), (u, ups.at[i]), (d, downs.at[i])):
            copies.append(pltpu.make_async_copy(src, dst, sems.at[len(copies)]))
    order = (0, 1, 3, 4, 2, 5)
    for i in order[:3]:
        copies[i].start()

    def wait(at):
        copies[order[at]].wait()
        if at + 3 < len(order):
            copies[order[at + 3]].start()

    rows = uncut(rows_ref[...])
    hidden = []
    for i in range(2):
        wait(2 * i)
        gate = jnp.dot(rows, gates[i], preferred_element_type=F32)
        wait(2 * i + 1)
        up = jnp.dot(rows, ups[i], preferred_element_type=F32)
        hidden.append((gate * jax.nn.sigmoid(1.702 * gate) * (up + 1.0)).astype(BF16))
    total = None
    for i in range(2):
        wait(4 + i)
        part = jnp.dot(hidden[i], downs[i], preferred_element_type=F32)
        total = part if total is None else total + part
    out_ref[...] = total.astype(out_ref.dtype)


def join_kernel(ours_ref, *refs):
    *theirs, out_ref = refs
    lines, width = out_ref.shape
    count = lines // CUTS
    line = lax.broadcasted_iota(jnp.int32, (lines, count), 0)
    row = lax.broadcasted_iota(jnp.int32, (lines, count), 1)
    total = jnp.concatenate([r[...] for r in theirs], axis=0).astype(F32) + ours_ref[...]
    total = total.astype(BF16)
    out = None
    for q in range(CUTS):
        put = jnp.where(line == row * CUTS + q, 1.0, 0.0).astype(BF16)
        part = jnp.dot(put, total[:, q * width : (q + 1) * width], preferred_element_type=F32)
        out = part if out is None else out + part
    out_ref[...] = out.astype(BF16)


def finish_kernel(tokens_ref, mix_ref, returned_ref, out_ref):
    core = lax.axis_index("tensor")
    own = out_ref.shape[0]
    parts = jnp.dot(mix_ref[...], uncut(returned_ref[...]), preferred_element_type=F32)
    weighted = parts[2 * own :] + parts[own : 2 * own] + parts[:own]
    resident = jnp.where(core == 0, tokens_ref[:own].astype(F32), tokens_ref[own:].astype(F32))
    out_ref[...] = (resident + weighted).astype(BF16)


def small(limit):
    return pltpu.CompilerParams(vmem_limit_bytes=limit * 2**20)


def ffn(rows, weights, dtype):
    depth, width = weights[0].shape
    flops = 12 * (rows.shape[0] // CUTS) * depth * width
    return pl.pallas_call(
        ffn_kernel,
        out_shape=jax.ShapeDtypeStruct((rows.shape[0] // CUTS, depth), dtype),
        in_specs=[VMEM] + [HBM] * 6,
        out_specs=VMEM,
        scratch_shapes=[
            pltpu.VMEM((2, depth, width), BF16),
            pltpu.VMEM((2, depth, width), BF16),
            pltpu.VMEM((2, width, depth), BF16),
            pltpu.SemaphoreType.DMA((6,)),
        ],
        compiler_params=pltpu.CompilerParams(vmem_limit_bytes=53200 * 1024),
        cost_estimate=pl.CostEstimate(flops=flops, bytes_accessed=12 * depth * width, transcendentals=0),
        name="ffn",
    )(rows, *weights)


def per_device(tokens, gain, route_ids, route_weights, w_gate, w_up, w_down):
    cores = lax.axis_size("tensor")
    peers = lax.axis_size("z") * lax.axis_size("pair")
    count, feats = tokens.shape
    own = count // cores
    room = max(2, own * route_ids.shape[1] // peers)
    lines, width = peers * room * CUTS, feats // CUTS
    ids, mixing = route_ids.T, route_weights.T
    packed = pl.pallas_call(
        functools.partial(pack_kernel, own, room),
        out_shape=jax.ShapeDtypeStruct((lines, width), BF16),
        in_specs=[HBM] * 3,
        out_specs=VMEM,
        scratch_shapes=[
            pltpu.VMEM(tokens.shape, tokens.dtype),
            pltpu.VMEM(gain.shape, gain.dtype),
            pltpu.VMEM(ids.shape, ids.dtype),
            pltpu.SemaphoreType.DMA((3,)),
        ],
        name="pack",
    )(tokens, gain, ids)
    blocks = (peers, room * CUTS, width)
    mine = lax.all_to_all(packed.reshape(blocks), ("z", "pair"), 0, 0, tiled=True)
    swap = [(0, 1), (1, 0)]
    held, late_ids, late_mixing, packed = lax.optimization_barrier(
        ((w_gate[0], w_up[0], w_down[0]), ids, mixing, packed)
    )
    mix = pl.pallas_call(
        functools.partial(mix_kernel, own, room),
        out_shape=jax.ShapeDtypeStruct((3 * own, peers * room), BF16),
        in_specs=[VMEM] * 2,
        out_specs=VMEM,
        compiler_params=small(8),
        name="mix",
    )(late_ids, late_mixing)
    sent = tuple(lax.ppermute(w, "tensor", swap) for w in held)
    mine, sent, mix = lax.optimization_barrier((mine, sent, mix))
    mine = mine.reshape(lines, width)
    weights = (*held, *sent)
    step = lines // CHUNKS
    theirs = [
        lax.ppermute(mine[i * step : (i + 1) * step], "half", swap) for i in range(CHUNKS)
    ]
    from_them = [lax.ppermute(ffn(rows, weights, BF16), "half", swap) for rows in theirs]
    ours = ffn(mine, weights, F32)
    summed = pl.pallas_call(
        join_kernel,
        out_shape=jax.ShapeDtypeStruct((lines, width), BF16),
        in_specs=[VMEM] * (1 + CHUNKS),
        out_specs=VMEM,
        compiler_params=small(8),
        name="join",
    )(ours, *from_them)
    returned = lax.all_to_all(summed.reshape(blocks), ("z", "pair"), 0, 0, tiled=True)
    finished = pl.pallas_call(
        finish_kernel,
        out_shape=jax.ShapeDtypeStruct((own, feats), BF16),
        in_specs=[VMEM] * 3,
        out_specs=VMEM,
        compiler_params=small(8),
        name="finish",
    )(tokens, mix, returned.reshape(lines, width))
    return lax.all_gather(finished, "tensor", axis=0, tiled=True)


def solution(mesh):
    parts = mesh.devices.shape
    grid = Mesh(
        mesh.devices.reshape(parts[0], -1, X // 2, 2, parts[2]),
        ("groups", "z", "pair", "half", "tensor"),
    )
    chips = ("z", "pair", "half")
    rows = P(("groups", *chips), None)
    placed = (
        rows,
        P(),
        rows,
        rows,
        P(chips, None, "tensor"),
        P(chips, None, "tensor"),
        P(chips, "tensor", None),
    )
    return jax.shard_map(
        per_device, mesh=grid, in_specs=placed, out_specs=rows, check_vma=False
    )
```

```python
import functools

import jax
import jax.numpy as jnp
from jax import lax
from jax.experimental import pallas as pl
from jax.experimental.pallas import tpu as pltpu
from jax.sharding import Mesh, PartitionSpec as P

X = 8
CUTS = 4
BLOCK = 256
VMEM = pl.BlockSpec(memory_space=pltpu.VMEM)
HBM = pl.BlockSpec(memory_space=pltpu.HBM)
F32 = jnp.float32
BF16 = jnp.bfloat16
ROWS_FIRST = (((0,), (0,)), ((), ()))


def split(index, by):
    if by & (by - 1) == 0:
        return lax.shift_right_logical(index, by.bit_length() - 1), index & (by - 1)
    quotient = lax.div(index, by)
    return quotient, index - quotient * by


def routing(own, room, cuts, lines, ids, weights):
    count = ids.shape[1] // cuts
    core = lax.axis_index("tensor")
    line = lax.broadcasted_iota(jnp.int32, (lines, cuts * count), 0)
    column = lax.broadcasted_iota(jnp.int32, (lines, cuts * count), 1)
    slot, cut = split(line, cuts)
    expert, position = split(slot, room)
    of_cut, token = split(column, count)
    named = jnp.zeros(line.shape, F32)
    value = jnp.zeros(line.shape, F32)
    for k in range(ids.shape[0]):
        hit = ids[k : k + 1, :] == expert
        named = named + jnp.where(hit, 1.0, 0.0)
        if weights is not None:
            value = value + jnp.where(hit, weights[k : k + 1, :], 0.0)
    first = lax.broadcasted_iota(jnp.int32, (cuts * count,) * 2, 0)
    second = lax.broadcasted_iota(jnp.int32, (cuts * count,) * 2, 1)
    same_block = split(first, own)[0] == split(second, own)[0]
    earlier = jnp.where((first < second) & same_block, 1.0, 0.0).astype(BF16)
    before = jnp.dot(named.astype(BF16), earlier, preferred_element_type=F32)
    here = (before == position.astype(F32)) & (split(token, own)[0] == core) & (of_cut == cut)
    return jnp.where(here, named if weights is None else value, 0.0)


def pack_kernel(own, room, tokens_hbm, gain_hbm, ids_hbm, packed_ref, tokens_ref, gain_ref, ids_ref, sems):
    copies = [
        pltpu.make_async_copy(src, dst, sems.at[i])
        for i, (src, dst) in enumerate(
            ((ids_hbm, ids_ref), (tokens_hbm, tokens_ref), (gain_hbm, gain_ref))
        )
    ]
    for copy in copies:
        copy.start()
    copies[0].wait()
    lines, width = packed_ref.shape
    ids = jnp.concatenate([ids_ref[...]] * CUTS, axis=1)
    chosen = routing(own, room, CUTS, lines, ids, None).astype(BF16)
    copies[1].wait()
    resident = tokens_ref[...].astype(F32)
    mean = jnp.mean(resident * resident, axis=1, keepdims=True)
    scaled = resident * lax.rsqrt(mean + 1e-05)
    copies[2].wait()
    normed = (scaled * gain_ref[...][None, :]).astype(BF16)
    stacked = jnp.concatenate([normed[:, q * width : (q + 1) * width] for q in range(CUTS)], axis=0)
    packed_ref[...] = jnp.dot(chosen, stacked, preferred_element_type=F32).astype(BF16)


def mix_kernel(own, room, ids_ref, weights_ref, mix_ref):
    core = lax.axis_index("tensor")
    slots = mix_ref.shape[1]
    mix = routing(own, room, 1, slots, ids_ref[...], weights_ref[...]).T
    mix = jnp.where(core == 0, mix[:own], mix[own:])
    high = mix.astype(BF16)
    rest = mix - high.astype(F32)
    mid = rest.astype(BF16)
    mix_ref[...] = jnp.concatenate([high, mid, (rest - mid.astype(F32)).astype(BF16)], axis=0)


def shuffle(size, back):
    to = lax.broadcasted_iota(jnp.int32, (size, size), 1 if back else 0)
    at = lax.broadcasted_iota(jnp.int32, (size, size), 0 if back else 1)
    row, cut = split(at, CUTS)
    return jnp.where(to == cut * (size // CUTS) + row, 1.0, 0.0).astype(BF16)


def uncut(held):
    lines, _ = held.shape
    size = min(BLOCK, lines)
    move, count = shuffle(size, False), size // CUTS
    rows = []
    for start in range(0, lines, size):
        block = jnp.dot(move, held[start : start + size], preferred_element_type=F32).astype(BF16)
        rows.append(
            jnp.concatenate([block[q * count : (q + 1) * count] for q in range(CUTS)], axis=1)
        )
    return jnp.concatenate(rows, axis=0)


def recut(rows):
    lines, width = rows.shape[0] * CUTS, rows.shape[1] // CUTS
    size = min(BLOCK, lines)
    move, count = shuffle(size, True), size // CUTS
    out = []
    for start in range(0, rows.shape[0], count):
        block = jnp.concatenate(
            [rows[start : start + count, q * width : (q + 1) * width] for q in range(CUTS)], axis=0
        )
        out.append(jnp.dot(move, block, preferred_element_type=F32).astype(BF16))
    return jnp.concatenate(out, axis=0)


def ffn_kernel(rows_ref, g0, u0, d0, g1, u1, d1, ours_ref, theirs_ref, gates, ups, downs, sems):
    copies = []
    for i, (g, u, d) in enumerate(((g0, u0, d0), (g1, u1, d1))):
        for src, dst in ((g, gates.at[i]), (u, ups.at[i]), (d, downs.at[i])):
            copies.append(pltpu.make_async_copy(src, dst, sems.at[len(copies)]))
    for i in (0, 1, 3, 4, 2, 5):
        copies[i].start()
    rows = uncut(rows_ref[...])
    hidden = []
    for i in range(2):
        copies[3 * i].wait()
        gate = jnp.dot(rows, gates[i], preferred_element_type=F32)
        copies[3 * i + 1].wait()
        up = jnp.dot(rows, ups[i], preferred_element_type=F32)
        hidden.append((gate * jax.nn.sigmoid(1.702 * gate) * (up + 1.0)).astype(BF16))
    total = None
    for i in range(2):
        copies[3 * i + 2].wait()
        part = jnp.dot(hidden[i], downs[i], preferred_element_type=F32)
        total = part if total is None else total + part
    low = lax.axis_index("half") == 0
    count = ours_ref.shape[0]
    ours_ref[...] = jnp.where(low, total[:count], total[count:])
    theirs_ref[...] = jnp.where(low, total[count:], total[:count]).astype(BF16)


def join_kernel(ours_ref, both_ref, out_ref):
    low = lax.axis_index("half") == 0
    count = ours_ref.shape[0]
    theirs = jnp.where(low, both_ref[count:].astype(F32), both_ref[:count].astype(F32))
    out_ref[...] = recut((ours_ref[...] + theirs).astype(BF16))


def finish_kernel(tokens_ref, mix_ref, returned_ref, out_ref):
    core = lax.axis_index("tensor")
    own = out_ref.shape[0]
    parts = jnp.dot(mix_ref[...], uncut(returned_ref[...]), preferred_element_type=F32)
    weighted = parts[2 * own :] + parts[own : 2 * own] + parts[:own]
    resident = jnp.where(core == 0, tokens_ref[:own].astype(F32), tokens_ref[own:].astype(F32))
    out_ref[...] = (resident + weighted).astype(BF16)


def small(limit):
    return pltpu.CompilerParams(vmem_limit_bytes=limit * 2**20)


def ffn(rows, weights):
    depth, width = weights[0].shape
    count = rows.shape[0] // CUTS
    flops = 12 * count * depth * width
    return pl.pallas_call(
        ffn_kernel,
        out_shape=(
            jax.ShapeDtypeStruct((count // 2, depth), F32),
            jax.ShapeDtypeStruct((count // 2, depth), BF16),
        ),
        in_specs=[VMEM] + [HBM] * 6,
        out_specs=(VMEM, VMEM),
        scratch_shapes=[
            pltpu.VMEM((2, depth, width), BF16),
            pltpu.VMEM((2, depth, width), BF16),
            pltpu.VMEM((2, width, depth), BF16),
            pltpu.SemaphoreType.DMA((6,)),
        ],
        compiler_params=pltpu.CompilerParams(vmem_limit_bytes=53200 * 1024),
        cost_estimate=pl.CostEstimate(flops=flops, bytes_accessed=12 * depth * width, transcendentals=0),
        name="ffn",
    )(rows, *weights)


def per_device(tokens, gain, route_ids, route_weights, w_gate, w_up, w_down):
    cores = lax.axis_size("tensor")
    peers = lax.axis_size("z") * lax.axis_size("pair")
    count, feats = tokens.shape
    own = count // cores
    room = max(2, own * route_ids.shape[1] // peers)
    lines, width = peers * room * CUTS, feats // CUTS
    ids, mixing = route_ids.T, route_weights.T
    packed = pl.pallas_call(
        functools.partial(pack_kernel, own, room),
        out_shape=jax.ShapeDtypeStruct((lines, width), BF16),
        in_specs=[HBM] * 3,
        out_specs=VMEM,
        scratch_shapes=[
            pltpu.VMEM(tokens.shape, tokens.dtype),
            pltpu.VMEM(gain.shape, gain.dtype),
            pltpu.VMEM(ids.shape, ids.dtype),
            pltpu.SemaphoreType.DMA((3,)),
        ],
        name="pack",
    )(tokens, gain, ids)
    blocks = (peers, room * CUTS, width)
    mine = lax.all_to_all(packed.reshape(blocks), ("z", "pair"), 0, 0, tiled=True)
    swap = [(0, 1), (1, 0)]
    held, late_ids, late_mixing, packed = lax.optimization_barrier(
        ((w_gate[0], w_up[0], w_down[0]), ids, mixing, packed)
    )
    mix = pl.pallas_call(
        functools.partial(mix_kernel, own, room),
        out_shape=jax.ShapeDtypeStruct((3 * own, peers * room), BF16),
        in_specs=[VMEM] * 2,
        out_specs=VMEM,
        compiler_params=small(8),
        name="mix",
    )(late_ids, late_mixing)
    sent = tuple(lax.ppermute(w, "tensor", swap) for w in held)
    mine, sent, mix = lax.optimization_barrier((mine, sent, mix))
    mine = mine.reshape(lines, width)
    weights = (*held, *sent)
    rows = lax.all_gather(mine, "half", axis=0, tiled=True)
    ours, theirs = ffn(rows, weights)
    both = lax.all_gather(theirs, "half", axis=0, tiled=True)
    summed = pl.pallas_call(
        join_kernel,
        out_shape=jax.ShapeDtypeStruct((lines, width), BF16),
        in_specs=[VMEM] * 2,
        out_specs=VMEM,
        compiler_params=small(8),
        name="join",
    )(ours, both)
    returned = lax.all_to_all(summed.reshape(blocks), ("z", "pair"), 0, 0, tiled=True)
    finished = pl.pallas_call(
        finish_kernel,
        out_shape=jax.ShapeDtypeStruct((own, feats), BF16),
        in_specs=[VMEM] * 3,
        out_specs=VMEM,
        compiler_params=small(8),
        name="finish",
    )(tokens, mix, returned.reshape(lines, width))
    return lax.all_gather(finished, "tensor", axis=0, tiled=True)


def solution(mesh):
    parts = mesh.devices.shape
    grid = Mesh(
        mesh.devices.reshape(parts[0], -1, X // 2, 2, parts[2]),
        ("groups", "z", "pair", "half", "tensor"),
    )
    chips = ("z", "pair", "half")
    rows = P(("groups", *chips), None)
    placed = (
        rows,
        P(),
        rows,
        rows,
        P(chips, None, "tensor"),
        P(chips, None, "tensor"),
        P(chips, "tensor", None),
    )
    return jax.shard_map(
        per_device, mesh=grid, in_specs=placed, out_specs=rows, check_vma=False
    )
```

```python
import functools

import jax
import jax.numpy as jnp
from jax import lax
from jax.experimental import pallas as pl
from jax.experimental.pallas import tpu as pltpu
from jax.sharding import Mesh, PartitionSpec as P

X = 8
CUTS = 4
BLOCK = 256
GRANT = 53200
VMEM = pl.BlockSpec(memory_space=pltpu.VMEM)
HBM = pl.BlockSpec(memory_space=pltpu.HBM)
F32 = jnp.float32
BF16 = jnp.bfloat16
ROWS_FIRST = (((0,), (0,)), ((), ()))


def split(index, by):
    if by & (by - 1) == 0:
        return lax.shift_right_logical(index, by.bit_length() - 1), index & (by - 1)
    quotient = lax.div(index, by)
    return quotient, index - quotient * by


def routing(own, room, cuts, lines, ids, weights):
    count = ids.shape[1] // cuts
    core = lax.axis_index("tensor")
    line = lax.broadcasted_iota(jnp.int32, (lines, cuts * count), 0)
    column = lax.broadcasted_iota(jnp.int32, (lines, cuts * count), 1)
    slot, cut = split(line, cuts)
    expert, position = split(slot, room)
    of_cut, token = split(column, count)
    named = jnp.zeros(line.shape, F32)
    value = jnp.zeros(line.shape, F32)
    for k in range(ids.shape[0]):
        hit = ids[k : k + 1, :] == expert
        named = named + jnp.where(hit, 1.0, 0.0)
        if weights is not None:
            value = value + jnp.where(hit, weights[k : k + 1, :], 0.0)
    first = lax.broadcasted_iota(jnp.int32, (cuts * count,) * 2, 0)
    second = lax.broadcasted_iota(jnp.int32, (cuts * count,) * 2, 1)
    same_block = split(first, own)[0] == split(second, own)[0]
    earlier = jnp.where((first < second) & same_block, 1.0, 0.0).astype(BF16)
    before = jnp.dot(named.astype(BF16), earlier, preferred_element_type=F32)
    here = (before == position.astype(F32)) & (split(token, own)[0] == core) & (of_cut == cut)
    return jnp.where(here, named if weights is None else value, 0.0)


def pack_kernel(own, room, tokens_hbm, gain_hbm, ids_hbm, packed_ref, tokens_ref, gain_ref, ids_ref, sems):
    copies = [
        pltpu.make_async_copy(src, dst, sems.at[i])
        for i, (src, dst) in enumerate(
            ((ids_hbm, ids_ref), (tokens_hbm, tokens_ref), (gain_hbm, gain_ref))
        )
    ]
    for copy in copies:
        copy.start()
    copies[0].wait()
    lines, width = packed_ref.shape
    ids = jnp.concatenate([ids_ref[...]] * CUTS, axis=1)
    chosen = routing(own, room, CUTS, lines, ids, None).astype(BF16)
    copies[1].wait()
    resident = tokens_ref[...].astype(F32)
    mean = jnp.mean(resident * resident, axis=1, keepdims=True)
    scaled = resident * lax.rsqrt(mean + 1e-05)
    copies[2].wait()
    normed = (scaled * gain_ref[...][None, :]).astype(BF16)
    stacked = jnp.concatenate([normed[:, q * width : (q + 1) * width] for q in range(CUTS)], axis=0)
    packed_ref[...] = jnp.dot(chosen, stacked, preferred_element_type=F32).astype(BF16)


def mix_kernel(own, room, ids_ref, weights_ref, mix_ref):
    core = lax.axis_index("tensor")
    slots = mix_ref.shape[1]
    mix = routing(own, room, 1, slots, ids_ref[...], weights_ref[...]).T
    mix = jnp.where(core == 0, mix[:own], mix[own:])
    high = mix.astype(BF16)
    rest = mix - high.astype(F32)
    mid = rest.astype(BF16)
    mix_ref[...] = jnp.concatenate([high, mid, (rest - mid.astype(F32)).astype(BF16)], axis=0)


def shuffle(size, back):
    to = lax.broadcasted_iota(jnp.int32, (size, size), 1 if back else 0)
    at = lax.broadcasted_iota(jnp.int32, (size, size), 0 if back else 1)
    row, cut = split(at, CUTS)
    return jnp.where(to == cut * (size // CUTS) + row, 1.0, 0.0).astype(BF16)


def uncut(held):
    lines, _ = held.shape
    size = min(BLOCK, lines)
    move, count = shuffle(size, False), size // CUTS
    rows = []
    for start in range(0, lines, size):
        block = jnp.dot(move, held[start : start + size], preferred_element_type=F32).astype(BF16)
        rows.append(
            jnp.concatenate([block[q * count : (q + 1) * count] for q in range(CUTS)], axis=1)
        )
    return jnp.concatenate(rows, axis=0)


def recut(rows):
    lines, width = rows.shape[0] * CUTS, rows.shape[1] // CUTS
    size = min(BLOCK, lines)
    move, count = shuffle(size, True), size // CUTS
    out = []
    for start in range(0, rows.shape[0], count):
        block = jnp.concatenate(
            [rows[start : start + count, q * width : (q + 1) * width] for q in range(CUTS)], axis=0
        )
        out.append(jnp.dot(move, block, preferred_element_type=F32).astype(BF16))
    return jnp.concatenate(out, axis=0)


def load(sources, buffers, sems):
    copies = []
    for i in range(2):
        for src, dst in zip(sources[3 * i : 3 * i + 3], buffers):
            copies.append(pltpu.make_async_copy(src, dst.at[i], sems.at[len(copies)]))
    for i in (0, 1, 3, 4, 2, 5):
        copies[i].start()
    return copies


def experts(rows, buffers, copies):
    gates, ups, downs = buffers
    hidden = []
    for i in range(2):
        copies[3 * i].wait()
        gate = jnp.dot(rows, gates[i], preferred_element_type=F32)
        copies[3 * i + 1].wait()
        up = jnp.dot(rows, ups[i], preferred_element_type=F32)
        hidden.append((gate * jax.nn.sigmoid(1.702 * gate) * (up + 1.0)).astype(BF16))
    total = None
    for i in range(2):
        copies[3 * i + 2].wait()
        part = jnp.dot(hidden[i], downs[i], preferred_element_type=F32)
        total = part if total is None else total + part
    return total


def first_kernel(mine_ref, *refs):
    *sources, early_ref, gates, ups, downs, sems = refs

    @pl.when(lax.axis_index("tensor") == 0)
    def _():
        copies = load(sources, (gates, ups, downs), sems)
        early_ref[...] = experts(uncut(mine_ref[...]), (gates, ups, downs), copies)


def second_kernel(rows_ref, *refs):
    *sources, ours_ref, theirs_ref, gates, ups, downs, sems = refs
    low = lax.axis_index("half") == 0
    core = lax.axis_index("tensor")
    count = ours_ref.shape[0]
    lines = rows_ref.shape[0] // 2
    buffers = (gates, ups, downs)

    @pl.when(core == 0)
    def _():
        copies = load(sources, buffers, sems)
        theirs = jnp.where(low, rows_ref[lines:], rows_ref[:lines])
        theirs_ref[...] = experts(uncut(theirs), buffers, copies).astype(BF16)

    @pl.when(core != 0)
    def _():
        copies = load(sources, buffers, sems)
        total = experts(uncut(rows_ref[...]), buffers, copies)
        ours_ref[...] = jnp.where(low, total[:count], total[count:])
        theirs_ref[...] = jnp.where(low, total[count:], total[:count]).astype(BF16)


def join_kernel(early_ref, ours_ref, both_ref, out_ref):
    low = lax.axis_index("half") == 0
    count = ours_ref.shape[0]
    theirs = jnp.where(low, both_ref[count:], both_ref[:count]).astype(F32)
    for core, own_ref in enumerate((early_ref, ours_ref)):

        @pl.when(lax.axis_index("tensor") == core)
        def _():
            out_ref[...] = recut((own_ref[...] + theirs).astype(BF16))


def finish_kernel(tokens_ref, mix_ref, returned_ref, out_ref):
    core = lax.axis_index("tensor")
    own = out_ref.shape[0]
    parts = jnp.dot(mix_ref[...], uncut(returned_ref[...]), preferred_element_type=F32)
    weighted = parts[2 * own :] + parts[own : 2 * own] + parts[:own]
    resident = jnp.where(core == 0, tokens_ref[:own].astype(F32), tokens_ref[own:].astype(F32))
    out_ref[...] = (resident + weighted).astype(BF16)


def small(limit):
    return pltpu.CompilerParams(vmem_limit_bytes=limit * 2**20)


def with_weights(kernel, rows, weights, out_shape, name):
    depth, width = weights[0].shape
    flops = 12 * (rows.shape[0] // CUTS) * depth * width
    return pl.pallas_call(
        kernel,
        out_shape=out_shape,
        in_specs=[VMEM] + [HBM] * 6,
        out_specs=[VMEM] * len(out_shape),
        scratch_shapes=[
            pltpu.VMEM((2, depth, width), BF16),
            pltpu.VMEM((2, depth, width), BF16),
            pltpu.VMEM((2, width, depth), BF16),
            pltpu.SemaphoreType.DMA((6,)),
        ],
        compiler_params=pltpu.CompilerParams(vmem_limit_bytes=GRANT * 1024),
        cost_estimate=pl.CostEstimate(flops=flops, bytes_accessed=12 * depth * width, transcendentals=0),
        name=name,
    )(rows, *weights)


def per_device(tokens, gain, route_ids, route_weights, w_gate, w_up, w_down):
    cores = lax.axis_size("tensor")
    peers = lax.axis_size("z") * lax.axis_size("pair")
    count, feats = tokens.shape
    own = count // cores
    room = max(2, own * route_ids.shape[1] // peers)
    lines, width = peers * room * CUTS, feats // CUTS
    ids, mixing = route_ids.T, route_weights.T
    packed = pl.pallas_call(
        functools.partial(pack_kernel, own, room),
        out_shape=jax.ShapeDtypeStruct((lines, width), BF16),
        in_specs=[HBM] * 3,
        out_specs=VMEM,
        scratch_shapes=[
            pltpu.VMEM(tokens.shape, tokens.dtype),
            pltpu.VMEM(gain.shape, gain.dtype),
            pltpu.VMEM(ids.shape, ids.dtype),
            pltpu.SemaphoreType.DMA((3,)),
        ],
        name="pack",
    )(tokens, gain, ids)
    blocks = (peers, room * CUTS, width)
    mine = lax.all_to_all(packed.reshape(blocks), ("z", "pair"), 0, 0, tiled=True)
    swap = [(0, 1), (1, 0)]
    held, late_ids, late_mixing, packed = lax.optimization_barrier(
        ((w_gate[0], w_up[0], w_down[0]), ids, mixing, packed)
    )
    mix = pl.pallas_call(
        functools.partial(mix_kernel, own, room),
        out_shape=jax.ShapeDtypeStruct((3 * own, peers * room), BF16),
        in_specs=[VMEM] * 2,
        out_specs=VMEM,
        compiler_params=small(8),
        name="mix",
    )(late_ids, late_mixing)
    sent = tuple(lax.ppermute(w, "tensor", swap) for w in held)
    mine, sent, mix = lax.optimization_barrier((mine, sent, mix))
    mine = mine.reshape(lines, width)
    weights = (*held, *sent)
    held_rows = (peers * room, feats)
    sums = jax.ShapeDtypeStruct(held_rows, F32)
    (early,) = with_weights(first_kernel, mine, weights, (sums,), "first")
    mine, early = lax.optimization_barrier((mine, early))
    rows = lax.all_gather(mine, "half", axis=0, tiled=True)
    ours, theirs = with_weights(
        second_kernel, rows, weights, (sums, jax.ShapeDtypeStruct(held_rows, BF16)), "second"
    )
    both = lax.all_gather(theirs, "half", axis=0, tiled=True)
    summed = pl.pallas_call(
        join_kernel,
        out_shape=jax.ShapeDtypeStruct((lines, width), BF16),
        in_specs=[VMEM] * 3,
        out_specs=VMEM,
        compiler_params=small(8),
        name="join",
    )(early, ours, both)
    returned = lax.all_to_all(summed.reshape(blocks), ("z", "pair"), 0, 0, tiled=True)
    finished = pl.pallas_call(
        finish_kernel,
        out_shape=jax.ShapeDtypeStruct((own, feats), BF16),
        in_specs=[VMEM] * 3,
        out_specs=VMEM,
        compiler_params=small(8),
        name="finish",
    )(tokens, mix, returned.reshape(lines, width))
    return lax.all_gather(finished, "tensor", axis=0, tiled=True)


def solution(mesh):
    parts = mesh.devices.shape
    grid = Mesh(
        mesh.devices.reshape(parts[0], -1, X // 2, 2, parts[2]),
        ("groups", "z", "pair", "half", "tensor"),
    )
    chips = ("z", "pair", "half")
    rows = P(("groups", *chips), None)
    placed = (
        rows,
        P(),
        rows,
        rows,
        P(chips, None, "tensor"),
        P(chips, None, "tensor"),
        P(chips, "tensor", None),
    )
    return jax.shard_map(
        per_device, mesh=grid, in_specs=placed, out_specs=rows, check_vma=False
    )
```

```python
import functools

import jax
import jax.numpy as jnp
from jax import lax
from jax.experimental import pallas as pl
from jax.experimental.pallas import tpu as pltpu
from jax.sharding import Mesh, PartitionSpec as P

X = 8
CUTS = 4
BLOCK = 256
GRANT = 53200
NEAR = 2
VMEM = pl.BlockSpec(memory_space=pltpu.VMEM)
HBM = pl.BlockSpec(memory_space=pltpu.HBM)
F32 = jnp.float32
BF16 = jnp.bfloat16
ROWS_FIRST = (((0,), (0,)), ((), ()))


def split(index, by):
    if by & (by - 1) == 0:
        return lax.shift_right_logical(index, by.bit_length() - 1), index & (by - 1)
    quotient = lax.div(index, by)
    return quotient, index - quotient * by


def routing(own, room, cuts, lines, ids, weights):
    count = ids.shape[1] // cuts
    core = lax.axis_index("tensor")
    line = lax.broadcasted_iota(jnp.int32, (lines, cuts * count), 0)
    column = lax.broadcasted_iota(jnp.int32, (lines, cuts * count), 1)
    slot, cut = split(line, cuts)
    expert, position = split(slot, room)
    of_cut, token = split(column, count)
    named = jnp.zeros(line.shape, F32)
    value = jnp.zeros(line.shape, F32)
    for k in range(ids.shape[0]):
        hit = ids[k : k + 1, :] == expert
        named = named + jnp.where(hit, 1.0, 0.0)
        if weights is not None:
            value = value + jnp.where(hit, weights[k : k + 1, :], 0.0)
    first = lax.broadcasted_iota(jnp.int32, (cuts * count,) * 2, 0)
    second = lax.broadcasted_iota(jnp.int32, (cuts * count,) * 2, 1)
    same_block = split(first, own)[0] == split(second, own)[0]
    earlier = jnp.where((first < second) & same_block, 1.0, 0.0).astype(BF16)
    before = jnp.dot(named.astype(BF16), earlier, preferred_element_type=F32)
    here = (before == position.astype(F32)) & (split(token, own)[0] == core) & (of_cut == cut)
    return jnp.where(here, named if weights is None else value, 0.0)


def pack_kernel(own, room, tokens_hbm, gain_hbm, ids_hbm, packed_ref, tokens_ref, gain_ref, ids_ref, sems):
    copies = [
        pltpu.make_async_copy(src, dst, sems.at[i])
        for i, (src, dst) in enumerate(
            ((ids_hbm, ids_ref), (tokens_hbm, tokens_ref), (gain_hbm, gain_ref))
        )
    ]
    for copy in copies:
        copy.start()
    copies[0].wait()
    lines, width = packed_ref.shape
    ids = jnp.concatenate([ids_ref[...]] * CUTS, axis=1)
    chosen = routing(own, room, CUTS, lines, ids, None).astype(BF16)
    copies[1].wait()
    resident = tokens_ref[...].astype(F32)
    mean = jnp.mean(resident * resident, axis=1, keepdims=True)
    scaled = resident * lax.rsqrt(mean + 1e-05)
    copies[2].wait()
    normed = (scaled * gain_ref[...][None, :]).astype(BF16)
    stacked = jnp.concatenate([normed[:, q * width : (q + 1) * width] for q in range(CUTS)], axis=0)
    packed_ref[...] = jnp.dot(chosen, stacked, preferred_element_type=F32).astype(BF16)


def mix_kernel(own, room, ids_ref, weights_ref, mix_ref):
    core = lax.axis_index("tensor")
    slots = mix_ref.shape[1]
    mix = routing(own, room, 1, slots, ids_ref[...], weights_ref[...]).T
    mix = jnp.where(core == 0, mix[:own], mix[own:])
    high = mix.astype(BF16)
    rest = mix - high.astype(F32)
    mid = rest.astype(BF16)
    mix_ref[...] = jnp.concatenate([high, mid, (rest - mid.astype(F32)).astype(BF16)], axis=0)


def shuffle(size, back):
    to = lax.broadcasted_iota(jnp.int32, (size, size), 1 if back else 0)
    at = lax.broadcasted_iota(jnp.int32, (size, size), 0 if back else 1)
    row, cut = split(at, CUTS)
    return jnp.where(to == cut * (size // CUTS) + row, 1.0, 0.0).astype(BF16)


def uncut(held):
    lines, _ = held.shape
    size = min(BLOCK, lines)
    move, count = shuffle(size, False), size // CUTS
    rows = []
    for start in range(0, lines, size):
        block = jnp.dot(move, held[start : start + size], preferred_element_type=F32).astype(BF16)
        rows.append(
            jnp.concatenate([block[q * count : (q + 1) * count] for q in range(CUTS)], axis=1)
        )
    return jnp.concatenate(rows, axis=0)


def recut(rows):
    lines, width = rows.shape[0] * CUTS, rows.shape[1] // CUTS
    size = min(BLOCK, lines)
    move, count = shuffle(size, True), size // CUTS
    out = []
    for start in range(0, rows.shape[0], count):
        block = jnp.concatenate(
            [rows[start : start + count, q * width : (q + 1) * width] for q in range(CUTS)], axis=0
        )
        out.append(jnp.dot(move, block, preferred_element_type=F32).astype(BF16))
    return jnp.concatenate(out, axis=0)


def load(sources, buffers, sems):
    copies = []
    for i in range(2):
        for src, dst in zip(sources[3 * i : 3 * i + 3], buffers):
            copies.append(pltpu.make_async_copy(src, dst.at[i], sems.at[len(copies)]))
    for i in (0, 1, 3, 4, 2, 5):
        copies[i].start()
    return copies


def experts(rows, buffers, copies):
    gates, ups, downs = buffers
    hidden = []
    for i in range(2):
        copies[3 * i].wait()
        gate = jnp.dot(rows, gates[i], preferred_element_type=F32)
        copies[3 * i + 1].wait()
        up = jnp.dot(rows, ups[i], preferred_element_type=F32)
        hidden.append((gate * jax.nn.sigmoid(1.702 * gate) * (up + 1.0)).astype(BF16))
    total = None
    for i in range(2):
        copies[3 * i + 2].wait()
        part = jnp.dot(hidden[i], downs[i], preferred_element_type=F32)
        total = part if total is None else total + part
    return total


def takes_own_first():
    z = lax.axis_index("z")
    inner = (z >= NEAR) & (z < lax.axis_size("z") - NEAR)
    return (lax.axis_index("tensor") == 0) & inner


def first_kernel(mine_ref, *refs):
    *sources, early_ref, gates, ups, downs, sems = refs

    @pl.when(takes_own_first())
    def _():
        copies = load(sources, (gates, ups, downs), sems)
        early_ref[...] = experts(uncut(mine_ref[...]), (gates, ups, downs), copies)


def second_kernel(rows_ref, *refs):
    *sources, ours_ref, theirs_ref, gates, ups, downs, sems = refs
    low = lax.axis_index("half") == 0
    own_first = takes_own_first()
    count = ours_ref.shape[0]
    lines = rows_ref.shape[0] // 2
    buffers = (gates, ups, downs)

    @pl.when(own_first)
    def _():
        copies = load(sources, buffers, sems)
        theirs = jnp.where(low, rows_ref[lines:], rows_ref[:lines])
        theirs_ref[...] = experts(uncut(theirs), buffers, copies).astype(BF16)

    @pl.when(jnp.logical_not(own_first))
    def _():
        copies = load(sources, buffers, sems)
        total = experts(uncut(rows_ref[...]), buffers, copies)
        ours_ref[...] = jnp.where(low, total[:count], total[count:])
        theirs_ref[...] = jnp.where(low, total[count:], total[:count]).astype(BF16)


def join_kernel(early_ref, ours_ref, both_ref, out_ref):
    low = lax.axis_index("half") == 0
    count = ours_ref.shape[0]
    theirs = jnp.where(low, both_ref[count:], both_ref[:count]).astype(F32)
    own_first = takes_own_first()
    for when, own_ref in ((own_first, early_ref), (jnp.logical_not(own_first), ours_ref)):

        @pl.when(when)
        def _():
            out_ref[...] = recut((own_ref[...] + theirs).astype(BF16))


def finish_kernel(tokens_ref, mix_ref, returned_ref, out_ref):
    core = lax.axis_index("tensor")
    own = out_ref.shape[0]
    parts = jnp.dot(mix_ref[...], uncut(returned_ref[...]), preferred_element_type=F32)
    weighted = parts[2 * own :] + parts[own : 2 * own] + parts[:own]
    resident = jnp.where(core == 0, tokens_ref[:own].astype(F32), tokens_ref[own:].astype(F32))
    out_ref[...] = (resident + weighted).astype(BF16)


def small(limit):
    return pltpu.CompilerParams(vmem_limit_bytes=limit * 2**20)


def with_weights(kernel, rows, weights, out_shape, name):
    depth, width = weights[0].shape
    flops = 12 * (rows.shape[0] // CUTS) * depth * width
    return pl.pallas_call(
        kernel,
        out_shape=out_shape,
        in_specs=[VMEM] + [HBM] * 6,
        out_specs=[VMEM] * len(out_shape),
        scratch_shapes=[
            pltpu.VMEM((2, depth, width), BF16),
            pltpu.VMEM((2, depth, width), BF16),
            pltpu.VMEM((2, width, depth), BF16),
            pltpu.SemaphoreType.DMA((6,)),
        ],
        compiler_params=pltpu.CompilerParams(vmem_limit_bytes=GRANT * 1024),
        cost_estimate=pl.CostEstimate(flops=flops, bytes_accessed=12 * depth * width, transcendentals=0),
        name=name,
    )(rows, *weights)


def per_device(tokens, gain, route_ids, route_weights, w_gate, w_up, w_down):
    cores = lax.axis_size("tensor")
    peers = lax.axis_size("z") * lax.axis_size("pair")
    count, feats = tokens.shape
    own = count // cores
    room = max(2, own * route_ids.shape[1] // peers)
    lines, width = peers * room * CUTS, feats // CUTS
    ids, mixing = route_ids.T, route_weights.T
    packed = pl.pallas_call(
        functools.partial(pack_kernel, own, room),
        out_shape=jax.ShapeDtypeStruct((lines, width), BF16),
        in_specs=[HBM] * 3,
        out_specs=VMEM,
        scratch_shapes=[
            pltpu.VMEM(tokens.shape, tokens.dtype),
            pltpu.VMEM(gain.shape, gain.dtype),
            pltpu.VMEM(ids.shape, ids.dtype),
            pltpu.SemaphoreType.DMA((3,)),
        ],
        name="pack",
    )(tokens, gain, ids)
    blocks = (peers, room * CUTS, width)
    mine = lax.all_to_all(packed.reshape(blocks), ("z", "pair"), 0, 0, tiled=True)
    swap = [(0, 1), (1, 0)]
    held, late_ids, late_mixing, packed = lax.optimization_barrier(
        ((w_gate[0], w_up[0], w_down[0]), ids, mixing, packed)
    )
    mix = pl.pallas_call(
        functools.partial(mix_kernel, own, room),
        out_shape=jax.ShapeDtypeStruct((3 * own, peers * room), BF16),
        in_specs=[VMEM] * 2,
        out_specs=VMEM,
        compiler_params=small(8),
        name="mix",
    )(late_ids, late_mixing)
    sent = tuple(lax.ppermute(w, "tensor", swap) for w in held)
    mine, sent, mix = lax.optimization_barrier((mine, sent, mix))
    mine = mine.reshape(lines, width)
    weights = (*held, *sent)
    held_rows = (peers * room, feats)
    sums = jax.ShapeDtypeStruct(held_rows, F32)
    (early,) = with_weights(first_kernel, mine, weights, (sums,), "first")
    mine, early = lax.optimization_barrier((mine, early))
    rows = lax.all_gather(mine, "half", axis=0, tiled=True)
    ours, theirs = with_weights(
        second_kernel, rows, weights, (sums, jax.ShapeDtypeStruct(held_rows, BF16)), "second"
    )
    both = lax.all_gather(theirs, "half", axis=0, tiled=True)
    summed = pl.pallas_call(
        join_kernel,
        out_shape=jax.ShapeDtypeStruct((lines, width), BF16),
        in_specs=[VMEM] * 3,
        out_specs=VMEM,
        compiler_params=small(8),
        name="join",
    )(early, ours, both)
    returned = lax.all_to_all(summed.reshape(blocks), ("z", "pair"), 0, 0, tiled=True)
    finished = pl.pallas_call(
        finish_kernel,
        out_shape=jax.ShapeDtypeStruct((own, feats), BF16),
        in_specs=[VMEM] * 3,
        out_specs=VMEM,
        compiler_params=small(8),
        name="finish",
    )(tokens, mix, returned.reshape(lines, width))
    return lax.all_gather(finished, "tensor", axis=0, tiled=True)


def solution(mesh):
    parts = mesh.devices.shape
    grid = Mesh(
        mesh.devices.reshape(parts[0], -1, X // 2, 2, parts[2]),
        ("groups", "z", "pair", "half", "tensor"),
    )
    chips = ("z", "pair", "half")
    rows = P(("groups", *chips), None)
    placed = (
        rows,
        P(),
        rows,
        rows,
        P(chips, None, "tensor"),
        P(chips, None, "tensor"),
        P(chips, "tensor", None),
    )
    return jax.shard_map(
        per_device, mesh=grid, in_specs=placed, out_specs=rows, check_vma=False
    )
```

```python
import functools

import jax
import jax.numpy as jnp
from jax import lax
from jax.experimental import pallas as pl
from jax.experimental.pallas import tpu as pltpu
from jax.sharding import Mesh, PartitionSpec as P

X = 8
CUTS = 4
BLOCK = 256
GRANT = 53200
VMEM = pl.BlockSpec(memory_space=pltpu.VMEM)
HBM = pl.BlockSpec(memory_space=pltpu.HBM)
F32 = jnp.float32
BF16 = jnp.bfloat16
ROWS_FIRST = (((0,), (0,)), ((), ()))


def split(index, by):
    if by & (by - 1) == 0:
        return lax.shift_right_logical(index, by.bit_length() - 1), index & (by - 1)
    quotient = lax.div(index, by)
    return quotient, index - quotient * by


def routing(own, room, cuts, lines, ids, weights):
    count = ids.shape[1] // cuts
    core = lax.axis_index("tensor")
    line = lax.broadcasted_iota(jnp.int32, (lines, cuts * count), 0)
    column = lax.broadcasted_iota(jnp.int32, (lines, cuts * count), 1)
    slot, cut = split(line, cuts)
    expert, position = split(slot, room)
    of_cut, token = split(column, count)
    named = jnp.zeros(line.shape, F32)
    value = jnp.zeros(line.shape, F32)
    for k in range(ids.shape[0]):
        hit = ids[k : k + 1, :] == expert
        named = named + jnp.where(hit, 1.0, 0.0)
        if weights is not None:
            value = value + jnp.where(hit, weights[k : k + 1, :], 0.0)
    first = lax.broadcasted_iota(jnp.int32, (cuts * count,) * 2, 0)
    second = lax.broadcasted_iota(jnp.int32, (cuts * count,) * 2, 1)
    same_block = split(first, own)[0] == split(second, own)[0]
    earlier = jnp.where((first < second) & same_block, 1.0, 0.0).astype(BF16)
    before = jnp.dot(named.astype(BF16), earlier, preferred_element_type=F32)
    here = (before == position.astype(F32)) & (split(token, own)[0] == core) & (of_cut == cut)
    return jnp.where(here, named if weights is None else value, 0.0)


def pack_kernel(own, room, tokens_hbm, gain_hbm, ids_hbm, packed_ref, tokens_ref, gain_ref, ids_ref, sems):
    copies = [
        pltpu.make_async_copy(src, dst, sems.at[i])
        for i, (src, dst) in enumerate(
            ((ids_hbm, ids_ref), (tokens_hbm, tokens_ref), (gain_hbm, gain_ref))
        )
    ]
    for copy in copies:
        copy.start()
    copies[0].wait()
    lines, width = packed_ref.shape
    ids = jnp.concatenate([ids_ref[...]] * CUTS, axis=1)
    chosen = routing(own, room, CUTS, lines, ids, None).astype(BF16)
    copies[1].wait()
    resident = tokens_ref[...].astype(F32)
    mean = jnp.mean(resident * resident, axis=1, keepdims=True)
    scaled = resident * lax.rsqrt(mean + 1e-05)
    copies[2].wait()
    normed = (scaled * gain_ref[...][None, :]).astype(BF16)
    stacked = jnp.concatenate([normed[:, q * width : (q + 1) * width] for q in range(CUTS)], axis=0)
    packed_ref[...] = jnp.dot(chosen, stacked, preferred_element_type=F32).astype(BF16)


def mix_kernel(own, room, ids_ref, weights_ref, mix_ref):
    core = lax.axis_index("tensor")
    slots = mix_ref.shape[1]
    mix = routing(own, room, 1, slots, ids_ref[...], weights_ref[...]).T
    mix = jnp.where(core == 0, mix[:own], mix[own:])
    high = mix.astype(BF16)
    rest = mix - high.astype(F32)
    mid = rest.astype(BF16)
    mix_ref[...] = jnp.concatenate([high, mid, (rest - mid.astype(F32)).astype(BF16)], axis=0)


def shuffle(size, back):
    to = lax.broadcasted_iota(jnp.int32, (size, size), 1 if back else 0)
    at = lax.broadcasted_iota(jnp.int32, (size, size), 0 if back else 1)
    row, cut = split(at, CUTS)
    return jnp.where(to == cut * (size // CUTS) + row, 1.0, 0.0).astype(BF16)


def uncut(held):
    lines, _ = held.shape
    size = min(BLOCK, lines)
    move, count = shuffle(size, False), size // CUTS
    rows = []
    for start in range(0, lines, size):
        block = jnp.dot(move, held[start : start + size], preferred_element_type=F32).astype(BF16)
        rows.append(
            jnp.concatenate([block[q * count : (q + 1) * count] for q in range(CUTS)], axis=1)
        )
    return jnp.concatenate(rows, axis=0)


def recut(rows):
    lines, width = rows.shape[0] * CUTS, rows.shape[1] // CUTS
    size = min(BLOCK, lines)
    move, count = shuffle(size, True), size // CUTS
    out = []
    for start in range(0, rows.shape[0], count):
        block = jnp.concatenate(
            [rows[start : start + count, q * width : (q + 1) * width] for q in range(CUTS)], axis=0
        )
        out.append(jnp.dot(move, block, preferred_element_type=F32).astype(BF16))
    return jnp.concatenate(out, axis=0)


def load(sources, buffers, sems):
    copies = []
    for i in range(2):
        for src, dst in zip(sources[3 * i : 3 * i + 3], buffers):
            copies.append(pltpu.make_async_copy(src, dst.at[i], sems.at[len(copies)]))
    for i in (0, 1, 3, 4):
        copies[i].start()
    return copies


def experts(rows, buffers, copies):
    gates, ups, downs = buffers
    hidden = []
    for i in range(2):
        copies[3 * i].wait()
        if i == 0:
            copies[2].start()
            copies[5].start()
        gate = jnp.dot(rows, gates[i], preferred_element_type=F32)
        copies[3 * i + 1].wait()
        up = jnp.dot(rows, ups[i], preferred_element_type=F32)
        hidden.append((gate * jax.nn.sigmoid(1.702 * gate) * (up + 1.0)).astype(BF16))
    total = None
    for i in range(2):
        copies[3 * i + 2].wait()
        part = jnp.dot(hidden[i], downs[i], preferred_element_type=F32)
        total = part if total is None else total + part
    return total


def first_kernel(mine_ref, *refs):
    *sources, early_ref, gates, ups, downs, sems = refs

    @pl.when(lax.axis_index("tensor") == 0)
    def _():
        copies = load(sources, (gates, ups, downs), sems)
        early_ref[...] = experts(uncut(mine_ref[...]), (gates, ups, downs), copies)


def second_kernel(rows_ref, *refs):
    *sources, ours_ref, theirs_ref, gates, ups, downs, sems = refs
    low = lax.axis_index("half") == 0
    core = lax.axis_index("tensor")
    count = ours_ref.shape[0]
    lines = rows_ref.shape[0] // 2
    buffers = (gates, ups, downs)

    @pl.when(core == 0)
    def _():
        copies = load(sources, buffers, sems)
        theirs = jnp.where(low, rows_ref[lines:], rows_ref[:lines])
        theirs_ref[...] = experts(uncut(theirs), buffers, copies).astype(BF16)

    @pl.when(core != 0)
    def _():
        copies = load(sources, buffers, sems)
        total = experts(uncut(rows_ref[...]), buffers, copies)
        ours_ref[...] = jnp.where(low, total[:count], total[count:])
        theirs_ref[...] = jnp.where(low, total[count:], total[:count]).astype(BF16)


def join_kernel(early_ref, ours_ref, both_ref, out_ref):
    low = lax.axis_index("half") == 0
    count = ours_ref.shape[0]
    theirs = jnp.where(low, both_ref[count:], both_ref[:count]).astype(F32)
    for core, own_ref in enumerate((early_ref, ours_ref)):

        @pl.when(lax.axis_index("tensor") == core)
        def _():
            out_ref[...] = recut((own_ref[...] + theirs).astype(BF16))


def finish_kernel(tokens_ref, mix_ref, returned_ref, out_ref):
    core = lax.axis_index("tensor")
    own = out_ref.shape[0]
    parts = jnp.dot(mix_ref[...], uncut(returned_ref[...]), preferred_element_type=F32)
    weighted = parts[2 * own :] + parts[own : 2 * own] + parts[:own]
    resident = jnp.where(core == 0, tokens_ref[:own].astype(F32), tokens_ref[own:].astype(F32))
    out_ref[...] = (resident + weighted).astype(BF16)


def small(limit):
    return pltpu.CompilerParams(vmem_limit_bytes=limit * 2**20)


def with_weights(kernel, rows, weights, out_shape, name):
    depth, width = weights[0].shape
    flops = 12 * (rows.shape[0] // CUTS) * depth * width
    return pl.pallas_call(
        kernel,
        out_shape=out_shape,
        in_specs=[VMEM] + [HBM] * 6,
        out_specs=[VMEM] * len(out_shape),
        scratch_shapes=[
            pltpu.VMEM((2, depth, width), BF16),
            pltpu.VMEM((2, depth, width), BF16),
            pltpu.VMEM((2, width, depth), BF16),
            pltpu.SemaphoreType.DMA((6,)),
        ],
        compiler_params=pltpu.CompilerParams(vmem_limit_bytes=GRANT * 1024),
        cost_estimate=pl.CostEstimate(flops=flops, bytes_accessed=12 * depth * width, transcendentals=0),
        name=name,
    )(rows, *weights)


def per_device(tokens, gain, route_ids, route_weights, w_gate, w_up, w_down):
    cores = lax.axis_size("tensor")
    peers = lax.axis_size("z") * lax.axis_size("pair")
    count, feats = tokens.shape
    own = count // cores
    room = max(2, own * route_ids.shape[1] // peers)
    lines, width = peers * room * CUTS, feats // CUTS
    ids, mixing = route_ids.T, route_weights.T
    packed = pl.pallas_call(
        functools.partial(pack_kernel, own, room),
        out_shape=jax.ShapeDtypeStruct((lines, width), BF16),
        in_specs=[HBM] * 3,
        out_specs=VMEM,
        scratch_shapes=[
            pltpu.VMEM(tokens.shape, tokens.dtype),
            pltpu.VMEM(gain.shape, gain.dtype),
            pltpu.VMEM(ids.shape, ids.dtype),
            pltpu.SemaphoreType.DMA((3,)),
        ],
        name="pack",
    )(tokens, gain, ids)
    blocks = (peers, room * CUTS, width)
    mine = lax.all_to_all(packed.reshape(blocks), ("z", "pair"), 0, 0, tiled=True)
    swap = [(0, 1), (1, 0)]
    held, late_ids, late_mixing, packed = lax.optimization_barrier(
        ((w_gate[0], w_up[0], w_down[0]), ids, mixing, packed)
    )
    mix = pl.pallas_call(
        functools.partial(mix_kernel, own, room),
        out_shape=jax.ShapeDtypeStruct((3 * own, peers * room), BF16),
        in_specs=[VMEM] * 2,
        out_specs=VMEM,
        compiler_params=small(8),
        name="mix",
    )(late_ids, late_mixing)
    sent = tuple(lax.ppermute(w, "tensor", swap) for w in held)
    mine, sent, mix = lax.optimization_barrier((mine, sent, mix))
    mine = mine.reshape(lines, width)
    weights = (*held, *sent)
    held_rows = (peers * room, feats)
    sums = jax.ShapeDtypeStruct(held_rows, F32)
    (early,) = with_weights(first_kernel, mine, weights, (sums,), "first")
    mine, early = lax.optimization_barrier((mine, early))
    rows = lax.all_gather(mine, "half", axis=0, tiled=True)
    ours, theirs = with_weights(
        second_kernel, rows, weights, (sums, jax.ShapeDtypeStruct(held_rows, BF16)), "second"
    )
    both = lax.all_gather(theirs, "half", axis=0, tiled=True)
    summed = pl.pallas_call(
        join_kernel,
        out_shape=jax.ShapeDtypeStruct((lines, width), BF16),
        in_specs=[VMEM] * 3,
        out_specs=VMEM,
        compiler_params=small(8),
        name="join",
    )(early, ours, both)
    returned = lax.all_to_all(summed.reshape(blocks), ("z", "pair"), 0, 0, tiled=True)
    finished = pl.pallas_call(
        finish_kernel,
        out_shape=jax.ShapeDtypeStruct((own, feats), BF16),
        in_specs=[VMEM] * 3,
        out_specs=VMEM,
        compiler_params=small(8),
        name="finish",
    )(tokens, mix, returned.reshape(lines, width))
    return lax.all_gather(finished, "tensor", axis=0, tiled=True)


def solution(mesh):
    parts = mesh.devices.shape
    grid = Mesh(
        mesh.devices.reshape(parts[0], -1, X // 2, 2, parts[2]),
        ("groups", "z", "pair", "half", "tensor"),
    )
    chips = ("z", "pair", "half")
    rows = P(("groups", *chips), None)
    placed = (
        rows,
        P(),
        rows,
        rows,
        P(chips, None, "tensor"),
        P(chips, None, "tensor"),
        P(chips, "tensor", None),
    )
    return jax.shard_map(
        per_device, mesh=grid, in_specs=placed, out_specs=rows, check_vma=False
    )
```
